256 devices in a mesh: gz: 64 (over x, z, core), gy: 4 (over y).
Axes of the slice: x: 4, y: 4, z: 8, core: 2. Of those that a mesh axis runs over, the one named last changes fastest.
Arguments:
- source_first: float32 [512, 32, 16, 128], P('gz', 'gy'), may hold values from -6 to 6
- source_second: float32 [256, 16, 16, 128], P('gz', 'gy'), may hold values from -6 to 6
- source_third: float32 [128, 8, 16, 128], P('gz', 'gy'), may hold values from -6 to 6
- source_fourth: float32 [64, 4, 16, 128], P('gz', 'gy'), may hold values from -6 to 6
- guess_first: float32 [512, 32, 16, 128], P('gz', 'gy'), may hold values from -6 to 6
- guess_second: float32 [256, 16, 16, 128], P('gz', 'gy'), may hold values from -6 to 6
- guess_third: float32 [128, 8, 16, 128], P('gz', 'gy'), may hold values from -6 to 6
- guess_fourth: float32 [64, 4, 16, 128], P('gz', 'gy'), may hold values from -6 to 6
- shift_first: float32 [512, 32, 128], P('gz', 'gy'), may hold values from 0.2 to 2
- shift_second: float32 [256, 16, 128], P('gz', 'gy'), may hold values from 0.2 to 2
- shift_third: float32 [128, 8, 128], P('gz', 'gy'), may hold values from 0.2 to 2
- shift_fourth: float32 [64, 4, 128], P('gz', 'gy'), may hold values from 0.2 to 2
- blocks_first: bfloat16 [512, 32, 2, 128, 128], P('gz', 'gy'), may hold values from -0.375 to 0.375
- blocks_second: bfloat16 [256, 16, 2, 128, 128], P('gz', 'gy'), may hold values from -0.375 to 0.375
- blocks_third: bfloat16 [128, 8, 2, 128, 128], P('gz', 'gy'), may hold values from -0.375 to 0.375
- links_first: int32 [512, 32, 2], P('gz', 'gy'), may hold values from 0 to 4095, as said below
- links_second: int32 [256, 16, 2], P('gz', 'gy'), may hold values from 0 to 1023, as said below
- links_third: int32 [128, 8, 2], P('gz', 'gy'), may hold values from 0 to 255, as said below
Outputs:
- smooth_first: float32 [512, 32, 16, 128], P('gz', 'gy')
- smooth_second: float32 [256, 16, 16, 128], P('gz', 'gy')
- smooth_third: float32 [128, 8, 16, 128], P('gz', 'gy')
- smooth_fourth: float32 [64, 4, 16, 128], P('gz', 'gy')
The draws below stay inside these ranges and needn't reach their ends.
Inputs may be any that keep to these rules, and one draw needn't show every extreme that they name: `links_first`: entry k of fine cell (i, j) names coarse column x * 16 + y with x within one of i // 2 and y within one of j // 2, both periodic on the coarse grid. `links_second`: entry k of cell (i, j) names coarse column x * 8 + y with x within one of i // 2 and y within one of j // 2, both periodic on the coarse grid. `links_third`: entry k of cell (i, j) names coarse column x * 4 + y with x within one of i // 2 and y within one of j // 2, both periodic on the coarse grid.
All inputs are finite; a program needn't handle non-finite values.
Results may differ from the reference program's by a relative error of at most 0.0005.
Values may be sent and summed in bfloat16 or wider, within the bound.
No kernel may reach another device: no remote copies, remote signals or barrier semaphores. Data moves between devices by JAX's collectives and lax.ppermute only.
A program may use at most 256 MiB of HBM per device.

```python
import math
import jax
import jax.numpy as jnp
from jax import lax

LINE = 128
SIDES = 16
LINKS = 2
DEGREE = 3
NX0 = 512
NY0 = 32
NX1 = 256
NY1 = 16
NX2 = 128
NY2 = 8
NX3 = 64
NY3 = 4


def column_links(key, fine_rows, fine_cols, coarse_rows, coarse_cols):
    offsets = jax.random.randint(jax.random.fold_in(key, 17), (fine_rows, fine_cols, LINKS, 2), -1, 2)
    row_index = (jnp.arange(fine_rows, dtype=jnp.int32) // 2)[:, None, None]
    col_index = (jnp.arange(fine_cols, dtype=jnp.int32) // 2)[None, :, None]
    coarse_row = (row_index + offsets[..., 0]) % coarse_rows
    coarse_col = (col_index + offsets[..., 1]) % coarse_cols
    return (coarse_row * coarse_cols + coarse_col).astype(jnp.int32)


def draw_links_first(key, part):
    return column_links(key, NX0, NY0, NX1, NY1)


def draw_links_second(key, part):
    return column_links(key, NX1, NY1, NX2, NY2)


def draw_links_third(key, part):
    return column_links(key, NX2, NY2, NX3, NY3)


def level_of(own_key, extent, shards, low, high):
    loudness = 1.0
    for position, shards_of in shards:
        draws = jax.random.uniform(jax.random.fold_in(jax.random.fold_in(own_key, 6), position), (shards_of,), jnp.float32, low / len(shards), high / len(shards))
        loudness = loudness * jnp.repeat(jnp.exp(draws), extent[position] // shards_of).reshape((-1,) + (1,) * (len(extent) - 1 - position))
    return loudness


def centred(key, shape, width, most, shards=(), held_as=jnp.bfloat16):
    factor_of = level_of(key, shape, shards, -0.22, 0.18) if shards else 1.0
    array = jax.random.normal(key, shape, jnp.float32) * width * factor_of
    return jnp.minimum(jnp.maximum(array, -most), most).astype(held_as)


def setup_inputs(seed: int = 0) -> dict:
    key_list = jax.random.split(jax.random.key(seed), 19)
    source_first = centred(key_list[0], (NX0, NY0, SIDES, LINE), 1.0, 6.0, ((0, 64), (1, 4)), jnp.float32)
    source_second = centred(key_list[1], (NX1, NY1, SIDES, LINE), 1.0, 6.0, ((0, 64), (1, 4)), jnp.float32)
    source_third = centred(key_list[2], (NX2, NY2, SIDES, LINE), 1.0, 6.0, ((0, 64), (1, 4)), jnp.float32)
    source_fourth = centred(key_list[3], (NX3, NY3, SIDES, LINE), 1.0, 6.0, ((0, 64), (1, 4)), jnp.float32)
    guess_first = centred(key_list[4], (NX0, NY0, SIDES, LINE), 1.0, 6.0, ((0, 64), (1, 4)), jnp.float32)
    guess_second = centred(key_list[5], (NX1, NY1, SIDES, LINE), 1.0, 6.0, ((0, 64), (1, 4)), jnp.float32)
    guess_third = centred(key_list[6], (NX2, NY2, SIDES, LINE), 1.0, 6.0, ((0, 64), (1, 4)), jnp.float32)
    guess_fourth = centred(key_list[7], (NX3, NY3, SIDES, LINE), 1.0, 6.0, ((0, 64), (1, 4)), jnp.float32)
    shift_first = jnp.clip(jnp.exp(math.log(2.0) - 2.3025851 * jax.random.uniform(key_list[8], (NX0, NY0, LINE), jnp.float32) ** level_of(key_list[8], (NX0, NY0, LINE), ((0, 64), (1, 4)), -0.2, 0.2)), 0.2, 2.0)
    shift_second = jnp.clip(jnp.exp(math.log(2.0) - 2.3025851 * jax.random.uniform(key_list[9], (NX1, NY1, LINE), jnp.float32) ** level_of(key_list[9], (NX1, NY1, LINE), ((0, 64), (1, 4)), -0.2, 0.2)), 0.2, 2.0)
    shift_third = jnp.clip(jnp.exp(math.log(2.0) - 2.3025851 * jax.random.uniform(key_list[10], (NX2, NY2, LINE), jnp.float32) ** level_of(key_list[10], (NX2, NY2, LINE), ((0, 64), (1, 4)), -0.2, 0.2)), 0.2, 2.0)
    shift_fourth = jnp.clip(jnp.exp(math.log(2.0) - 2.3025851 * jax.random.uniform(key_list[11], (NX3, NY3, LINE), jnp.float32) ** level_of(key_list[11], (NX3, NY3, LINE), ((0, 64), (1, 4)), -0.2, 0.2)), 0.2, 2.0)
    blocks_first = centred(key_list[12], (NX0, NY0, LINKS, LINE, LINE), (LINKS * LINE) ** -0.5, 0.375, ((0, 64), (1, 4)))
    blocks_second = centred(key_list[13], (NX1, NY1, LINKS, LINE, LINE), (LINKS * LINE) ** -0.5, 0.375, ((0, 64), (1, 4)))
    blocks_third = centred(key_list[14], (NX2, NY2, LINKS, LINE, LINE), (LINKS * LINE) ** -0.5, 0.375, ((0, 64), (1, 4)))
    links_first = draw_links_first(jax.random.fold_in(key_list[18], 71), 0)
    links_second = draw_links_second(jax.random.fold_in(key_list[18], 71), 0)
    links_third = draw_links_third(jax.random.fold_in(key_list[18], 71), 0)
    return {"source_first": source_first, "source_second": source_second, "source_third": source_third, "source_fourth": source_fourth, "guess_first": guess_first, "guess_second": guess_second, "guess_third": guess_third, "guess_fourth": guess_fourth, "shift_first": shift_first, "shift_second": shift_second, "shift_third": shift_third, "shift_fourth": shift_fourth, "blocks_first": blocks_first, "blocks_second": blocks_second, "blocks_third": blocks_third, "links_first": links_first, "links_second": links_second, "links_third": links_third}


upper_edge = 14.0
lower_edge = upper_edge / 8.0


def operate(vector, diagonal):
    beside = jnp.roll(vector, 1, 0) + jnp.roll(vector, -1, 0)
    beside = beside + jnp.roll(vector, 1, 1) + jnp.roll(vector, -1, 1)
    beside = beside + jnp.roll(vector, 1, 3) + jnp.roll(vector, -1, 3)
    return (6.0 + diagonal[:, :, None, :]) * vector - beside


def chebyshev(source, initial, diagonal):
    centre = (upper_edge + lower_edge) / 2.0
    half_width = (upper_edge - lower_edge) / 2.0
    ratio_edge = centre / half_width
    factor = 1.0 / ratio_edge
    residual = source - operate(initial, diagonal)
    direction = residual / centre
    result = initial
    for sweep_index in range(DEGREE):
        result = result + direction
        if sweep_index + 1 < DEGREE:
            residual = residual - operate(direction, diagonal)
            factor_next = 1.0 / (2.0 * ratio_edge - factor)
            direction = factor_next * factor * direction + (2.0 * factor_next / half_width) * residual
            factor = factor_next
    return result


def prolong(coarse, link_ids, blocks):
    coarse_lines = coarse.astype(jnp.bfloat16).reshape((-1,) + coarse.shape[2:])

    def one_row(row_pair):
        row_links, row_blocks = row_pair
        picked = coarse_lines[row_links].astype(jnp.float32)
        return jnp.einsum("bkrj,bkij->bri", picked, row_blocks.astype(jnp.float32),
                          precision=lax.Precision.HIGHEST)

    return lax.map(one_row, (link_ids, blocks))


def reference(source_first, source_second, source_third, source_fourth,
              guess_first, guess_second, guess_third, guess_fourth,
              shift_first, shift_second, shift_third, shift_fourth,
              blocks_first, blocks_second, blocks_third,
              links_first, links_second, links_third):
    smooth_fourth = chebyshev(source_fourth, guess_fourth, shift_fourth)
    start_third = guess_third + prolong(smooth_fourth, links_third, blocks_third)
    smooth_third = chebyshev(source_third, start_third, shift_third)
    start_second = guess_second + prolong(smooth_third, links_second, blocks_second)
    smooth_second = chebyshev(source_second, start_second, shift_second)
    start_first = guess_first + prolong(smooth_second, links_first, blocks_first)
    smooth_first = chebyshev(source_first, start_first, shift_first)
    return (smooth_first, smooth_second, smooth_third, smooth_fourth)
```

```python
import jax
import jax.numpy as jnp
from jax import lax
from jax.experimental import pallas as pl
from jax.experimental.pallas import tpu as pltpu
from jax.sharding import PartitionSpec as P

UPPER = 14.0
LOWER = UPPER / 8.0
CENTRE = (UPPER + LOWER) / 2.0
HALF = (UPPER - LOWER) / 2.0
RATIO = CENTRE / HALF
FACTOR0 = 1.0 / RATIO
FACTOR1 = 1.0 / (2.0 * RATIO - FACTOR0)
FACTOR2 = 1.0 / (2.0 * RATIO - FACTOR1)

F32 = jnp.float32
BF16 = jnp.bfloat16
R = 16
L = 128

NZ, NY = 64, 4


def swap(x, axis, partner):
    return lax.ppermute(x, axis, [(i, partner(i)) for i in range(lax.axis_size(axis))])


def z_on(x):
    return swap(x, "gz", lambda i: i ^ 1)


def z_off(x):
    return swap(x, "gz", lambda i: (((i + 1) ^ 1) - 1) % NZ)


def z_off3(x):
    return swap(x, "gz", lambda i: (i - 3 if i % 2 == 0 else i + 3) % NZ)


def y_by(x, k):
    return swap(x, "gy", lambda j: j ^ k)


def y_even(x):
    return y_by(x, 1)


def y_odd(x):
    return y_by(x, 3)


def neighbours(v, i, j, width, wrap):
    jl = (j - 1) % width if wrap else j - 1
    jr = (j + 1) % width if wrap else j + 1
    mid = v[i, j]
    beside = v[i - 1, j] + v[i + 1, j] + v[i, jl] + v[i, jr]
    beside = beside + pltpu.roll(mid, 1, 1) + pltpu.roll(mid, L - 1, 1)
    return mid, beside


def smooth(u, f, s, res, d0, d1, emit, low, rows, width, wrap):
    def columns(k):
        return range(width) if wrap else range(k, width - k)

    def first(i, carry):
        for j in columns(1):
            mid, beside = neighbours(u, i, j, width, wrap)
            r = f[i, j] - ((6.0 + s[i, j]) * mid - beside)
            res[i, j] = r
            d0[i, j] = r * (1.0 / CENTRE)
        return carry

    def second(i, carry):
        for j in columns(2):
            mid, beside = neighbours(d0, i, j, width, wrap)
            r = res[i, j] - ((6.0 + s[i, j]) * mid - beside)
            res[i, j] = r
            d1[i, j] = (FACTOR1 * FACTOR0) * mid + (2.0 * FACTOR1 / HALF) * r
        return carry

    def third(i, carry):
        for j in columns(3):
            mid, beside = neighbours(d1, i, j, width, wrap)
            r = res[i, j] - ((6.0 + s[i, j]) * mid - beside)
            d2 = (FACTOR2 * FACTOR1) * mid + (2.0 * FACTOR2 / HALF) * r
            emit(i, j, u[i, j] + d0[i, j] + mid + d2)
        return carry

    lax.fori_loop(low + 1, low + 5 + rows, first, 0)
    lax.fori_loop(low + 2, low + 4 + rows, second, 0)
    lax.fori_loop(low + 3, low + 3 + rows, third, 0)


def prolong_cell(lines, index, blocks, guess, a, b):
    total = guess[a, b]
    for k in range(2):
        ri, ci = index(a, b, k)
        total = total + lax.dot_general(
            lines[ri, ci], blocks[a, b, k], (((1,), (1,)), ((), ())), preferred_element_type=F32
        )
    return total


VMEM = pl.BlockSpec(memory_space=pltpu.VMEM)
SMEM = pl.BlockSpec(memory_space=pltpu.SMEM)


def call(kernel, inputs, specs, outs, scratch, name, flops):
    nbytes = sum(x.size * x.dtype.itemsize for x in inputs)
    return pl.pallas_call(
        kernel,
        out_shape=outs,
        in_specs=specs,
        out_specs=jax.tree.map(lambda _: VMEM, outs),
        scratch_shapes=scratch,
        name=name,
        cost_estimate=pl.CostEstimate(flops=flops, bytes_accessed=nbytes, transcendentals=0),
    )(*inputs)


def cells(rows, cols, dtype=F32):
    return pltpu.VMEM((rows, cols, R, L), dtype)


def shifts(rows, cols):
    return pltpu.VMEM((rows, cols, 1, L), F32)


def fourth_kernel(pair, a, a3, b, b3, links, blocks, guess, out, start, u, f, s, res, d0, d1, lines):
    gz, gy = lax.axis_index("gz"), lax.axis_index("gy")
    core = lax.rem(gz, 2)

    def place(ref, chip, first_bit):
        for slot in range(2):
            bit = first_bit if slot == 0 else 1 - first_bit
            row = chip * 2 + bit
            for k in range(4):
                col = lax.bitwise_xor(gy, k)
                f[row, col] = ref[slot, k, 0:16, :]
                u[row, col] = ref[slot, k, 16:32, :]
                s[row, col] = ref[slot, k, 32:33, :]

    place(pair, 2, core)
    place(a, 1 + 2 * core, 1 - core)
    place(b, 3 - 2 * core, core)
    place(a3, 4 * core, 1 - core)
    place(b3, 4 - 4 * core, core)

    def emit(i, j, value):
        lines[i - 3 - core, j] = value.astype(BF16)
        res[i, j] = value

    smooth(u, f, s, res, d0, d1, emit, core, 3, 4, True)
    out[0, 0] = res[4 + core, gy]

    def index(i, j, k):
        q = links[(i * 2 + j) * 2 + k]
        return lax.rem(q // 4 - gz + 1 + NZ, NZ), lax.rem(q, 4)

    for i in range(2):
        for j in range(2):
            start[i, j] = prolong_cell(lines, index, blocks, guess, i, j)


def third_kernel(pair, a, b, fpair, fa, fb, links, blocks, guess, out, start, u, f, s, res, d0, d1, lines):
    gz, gy = lax.axis_index("gz"), lax.axis_index("gy")
    core = lax.rem(gz, 2)

    def place(ref, fref, chip, first_bit):
        for slot in range(2):
            bit = first_bit if slot == 0 else 1 - first_bit
            for k in range(4):
                col = lax.bitwise_xor(gy, k) * 2
                for i in range(2):
                    row = chip * 4 + bit * 2 + i
                    for j in range(2):
                        at = (i * 2 + j) * R
                        u[row, col + j] = ref[slot, k, at : at + R, :]
                        f[row, col + j] = fref[slot, k, 40 + at : 40 + at + R, :]
                        s[row, col + j] = fref[slot, k, 33 + i * 2 + j : 34 + i * 2 + j, :]

    place(pair, fpair, 1, core)
    place(a, fa, 2 * core, 1 - core)
    place(b, fb, 2 - 2 * core, core)

    def emit(i, j, value):
        lines[i - 3 - 2 * core, j] = value.astype(BF16)
        res[i, j] = value

    smooth(u, f, s, res, d0, d1, emit, 2 * core, 4, 8, True)
    for i in range(2):
        for j in range(2):
            out[i, j] = res[4 + 2 * core + i, 2 * gy + j]

    def index(i, j, k):
        q = links[(i * 4 + j) * 2 + k]
        return lax.rem(q // 8 - 2 * gz + 1 + 2 * NZ, 2 * NZ), lax.rem(q, 8)

    for i in range(4):
        for j in range(4):
            start[i, j] = prolong_cell(lines, index, blocks, guess, i, j)


def second_kernel(own, on, off, fown, fon, foff, links, blocks, guess, out, start, even, odd, u, f, s, res, d0, d1, lines):
    gz, gy = lax.axis_index("gz"), lax.axis_index("gy")
    core, side = lax.rem(gz, 2), lax.rem(gy, 2)
    starts = (4, 8 - 8 * side, 8 * side)

    def place(ref, fref, row0):
        for k in range(3):
            for i in range(4):
                for j in range(4):
                    c = i * 4 + j
                    row, col = row0 + i, starts[k] + j
                    u[row, col] = ref[k, c * R : (c + 1) * R, :]
                    f[row, col] = fref[k, c * R : (c + 1) * R, :].astype(F32)
                    s[row, col] = fref[k, 256 + c : 257 + c, :].astype(F32)

    place(own, fown, 4)
    place(on, fon, 8 - 8 * core)
    place(off, foff, 8 * core)

    def emit(i, j, value):
        lines[i - 3, j - 3] = value.astype(BF16)
        res[i, j] = value

    smooth(u, f, s, res, d0, d1, emit, 0, 6, 12, False)
    for i in range(4):
        for j in range(4):
            out[i, j] = res[4 + i, 4 + j]

    def index(i, j, k):
        q = links[(i * 8 + j) * 2 + k]
        row = lax.rem(q // 16 - 4 * gz + 1 + 4 * NZ, 4 * NZ)
        return row, lax.rem(lax.rem(q, 16) - 4 * gy + 1 + 4 * NY, 4 * NY)

    def row_of_cells(i, carry):
        for j in range(8):
            start[i, j] = prolong_cell(lines, index, blocks, guess, i, j)
        return carry

    lax.fori_loop(0, 8, row_of_cells, 0)
    for i in range(8):
        for j in range(3):
            even[i, j] = start[i, 5 - 5 * side + j]
            odd[i, j] = start[i, 5 * side + j]


def first_kernel(own, even, odd, on, off, fown, feven, fodd, fon, foff, sown, seven, sodd, son, soff, out, u, f, s, res, d0, d1):
    gz, gy = lax.axis_index("gz"), lax.axis_index("gy")
    core, side = lax.rem(gz, 2), lax.rem(gy, 2)
    even_u, odd_u = 11 - 11 * side, 11 * side
    even_f, odd_f = 11 - 10 * side, 1 + 10 * side

    def own_rows(i, carry):
        for j in range(8):
            u[3 + i, 3 + j] = own[i, j]
            f[3 + i, 3 + j] = fown[i, j]
            s[3 + i, 3 + j] = sown[i, j : j + 1, :]
        for j in range(3):
            u[3 + i, even_u + j] = even[i, j]
            u[3 + i, odd_u + j] = odd[i, j]
        for j in range(2):
            f[3 + i, even_f + j] = feven[i, j].astype(F32)
            f[3 + i, odd_f + j] = fodd[i, j].astype(F32)
            s[3 + i, even_f + j] = seven[i, j : j + 1, :].astype(F32)
            s[3 + i, odd_f + j] = sodd[i, j : j + 1, :].astype(F32)
        return carry

    lax.fori_loop(0, 8, own_rows, 0)

    def place(ref, fref, sref, row_u, row_f):
        for i in range(3):
            for j in range(8):
                u[row_u + i, 3 + j] = ref[i, j]
            for j in range(3):
                u[row_u + i, even_u + j] = ref[i, 8 + j]
                u[row_u + i, odd_u + j] = ref[i, 11 + j]
        for i in range(2):
            for j in range(8):
                f[row_f + i, 3 + j] = fref[i, j].astype(F32)
                s[row_f + i, 3 + j] = sref[i, j : j + 1, :].astype(F32)
            for j in range(2):
                f[row_f + i, even_f + j] = fref[i, 8 + j].astype(F32)
                f[row_f + i, odd_f + j] = fref[i, 10 + j].astype(F32)
                s[row_f + i, even_f + j] = sref[i, 8 + j : 9 + j, :].astype(F32)
                s[row_f + i, odd_f + j] = sref[i, 10 + j : 11 + j, :].astype(F32)

    place(on, fon, son, 11 - 11 * core, 11 - 10 * core)
    place(off, foff, soff, 11 * core, 1 + 10 * core)

    def emit(i, j, value):
        out[i - 3, j - 3] = value

    smooth(u, f, s, res, d0, d1, emit, 0, 8, 14, False)


def strip(x, dim, at, width):
    return lax.dynamic_slice_in_dim(x, at, width, dim)


def sds(*shape, dtype=F32):
    return jax.ShapeDtypeStruct(shape, dtype)


def flat(x):
    return x.reshape(-1, L)


def shards(
    source_first, source_second, source_third, source_fourth,
    guess_first, guess_second, guess_third, guess_fourth,
    shift_first, shift_second, shift_third, shift_fourth,
    blocks_first, blocks_second, blocks_third,
    links_first, links_second, links_third,
):
    core = lax.axis_index("gz") % 2
    side = lax.axis_index("gy") % 2

    pack = jnp.concatenate(
        [flat(source_fourth), flat(guess_fourth), flat(shift_fourth), flat(shift_third), jnp.zeros((3, L), F32), flat(source_third)]
    )
    line = jnp.stack([pack, y_by(pack, 1), y_by(pack, 2), y_by(pack, 3)])
    pair = jnp.stack([line, z_on(line)])
    far = z_off3(pair[:, :, :40])
    near = z_off(pair)
    near_b, far_b = z_on(near), z_on(far)

    second = jnp.concatenate([flat(source_second), flat(shift_second)])
    f_even = strip(source_first, 1, 6 - 6 * side, 2)
    f_odd = strip(source_first, 1, 6 * side, 2)
    s_even = strip(shift_first, 1, 6 - 6 * side, 2)
    s_odd = strip(shift_first, 1, 6 * side, 2)
    ahead_even = y_even(jnp.concatenate([second, flat(f_even), flat(s_even)]))
    ahead_odd = y_odd(jnp.concatenate([second, flat(f_odd), flat(s_odd)]))
    second_even, second_odd = ahead_even[:272], ahead_odd[:272]
    f_even, f_odd = (x[272:528].reshape(8, 2, R, L) for x in (ahead_even, ahead_odd))
    s_even, s_odd = (x[528:544].reshape(8, 2, L) for x in (ahead_even, ahead_odd))
    second3 = jnp.stack([second, second_even, second_odd])

    def across(at):
        f = jnp.concatenate([strip(x, 0, at, 2) for x in (source_first, f_even, f_odd)], axis=1)
        s = jnp.concatenate([strip(x, 0, at, 2) for x in (shift_first, s_even, s_odd)], axis=1)
        return jnp.concatenate([flat(second3), flat(f), flat(s)])

    ahead_on = z_on(across(6 - 6 * core))
    ahead_off = z_off(across(6 * core))
    second_on, second_off = (x[:816].reshape(3, 272, L) for x in (ahead_on, ahead_off))
    f_on, f_off = (x[816:1200].reshape(2, 12, R, L) for x in (ahead_on, ahead_off))
    s_on, s_off = (x[1200:1224].reshape(2, 12, L) for x in (ahead_on, ahead_off))

    def smoothing_scratch(rows, cols):
        return [cells(rows, cols), cells(rows, cols), shifts(rows, cols)] + [cells(rows, cols)] * 3

    out_fourth, start_third = call(
        fourth_kernel,
        (pair, near, far, near_b, far_b, links_third.reshape(-1), blocks_third, guess_third),
        [VMEM] * 5 + [SMEM] + [VMEM] * 2,
        (sds(1, 1, R, L), sds(2, 2, R, L)),
        smoothing_scratch(10, 4) + [cells(3, 4, BF16)],
        "fourth", 4_000_000,
    )

    mine = flat(start_third)
    line3 = jnp.stack([mine, y_by(mine, 1), y_by(mine, 2), y_by(mine, 3)])
    pair3 = jnp.stack([line3, z_on(line3)])
    near3 = z_off(pair3)
    near3_b = z_on(near3)
    out_third, start_second = call(
        third_kernel,
        (pair3, near3, near3_b, pair, near, near_b, links_second.reshape(-1), blocks_second, guess_second),
        [VMEM] * 6 + [SMEM] + [VMEM] * 2,
        (sds(2, 2, R, L), sds(4, 4, R, L)),
        smoothing_scratch(12, 8) + [cells(4, 8, BF16)],
        "third", 8_000_000,
    )

    mine = flat(start_second)
    own2 = jnp.stack([mine, y_even(mine), y_odd(mine)])
    out_second, start_first, strip_even, strip_odd = call(
        second_kernel,
        (own2, z_on(own2), z_off(own2), second3, second_on, second_off, links_first.reshape(-1), blocks_first, guess_first),
        [VMEM] * 6 + [SMEM] + [VMEM] * 2,
        (sds(4, 4, R, L), sds(8, 8, R, L), sds(8, 3, R, L), sds(8, 3, R, L)),
        smoothing_scratch(12, 12) + [cells(6, 6, BF16)],
        "second", 16_000_000,
    )

    u_even, u_odd = y_even(strip_even), y_odd(strip_odd)

    def rows_of(at):
        return jnp.concatenate([strip(x, 0, at, 3) for x in (start_first, u_even, u_odd)], axis=1)

    u_on = z_on(rows_of(5 - 5 * core))
    u_off = z_off(rows_of(5 * core))
    (out_first,) = call(
        first_kernel,
        (start_first, u_even, u_odd, u_on, u_off, source_first, f_even, f_odd, f_on, f_off, shift_first, s_even, s_odd, s_on, s_off),
        [VMEM] * 15,
        (sds(8, 8, R, L),),
        smoothing_scratch(14, 14),
        "first", 16_000_000,
    )
    return out_first, out_second, out_third, out_fourth


def solution(mesh):
    field = P("gz", "gy", None, None)
    line = P("gz", "gy", None)
    block = P("gz", "gy", None, None, None)
    return jax.shard_map(
        shards,
        mesh=mesh,
        in_specs=(field,) * 8 + (line,) * 4 + (block,) * 3 + (line,) * 3,
        out_specs=(field,) * 4,
        check_vma=False,
    )
```

```python
import jax
import jax.numpy as jnp
from jax import lax
from jax.experimental import pallas as pl
from jax.experimental.pallas import tpu as pltpu
from jax.sharding import PartitionSpec as P


UPPER = 14.0
LOWER = UPPER / 8.0
CENTRE = (UPPER + LOWER) / 2.0
HALF = (UPPER - LOWER) / 2.0
RATIO = CENTRE / HALF
FACTOR0 = 1.0 / RATIO
FACTOR1 = 1.0 / (2.0 * RATIO - FACTOR0)
FACTOR2 = 1.0 / (2.0 * RATIO - FACTOR1)

F32 = jnp.float32
BF16 = jnp.bfloat16
R = 16
L = 128

NZ, NY = 64, 4


def swap(x, axis, partner):
    return lax.ppermute(x, axis, [(i, partner(i)) for i in range(lax.axis_size(axis))])


def z_on(x):
    return swap(x, "gz", lambda i: i ^ 1)


def z_off(x):
    return swap(x, "gz", lambda i: (((i + 1) ^ 1) - 1) % NZ)


def z_off3(x):
    return swap(x, "gz", lambda i: (i - 3 if i % 2 == 0 else i + 3) % NZ)


def y_by(x, k):
    return swap(x, "gy", lambda j: j ^ k)


def y_even(x):
    return y_by(x, 1)


def y_odd(x):
    return y_by(x, 3)


def neighbours(v, i, j, width, wrap):
    jl = (j - 1) % width if wrap else j - 1
    jr = (j + 1) % width if wrap else j + 1
    mid = v[i, j]
    beside = v[i - 1, j] + v[i + 1, j] + v[i, jl] + v[i, jr]
    beside = beside + pltpu.roll(mid, 1, 1) + pltpu.roll(mid, L - 1, 1)
    return mid, beside


def smooth(u, f, s, res, d0, d1, emit, low, rows, width, wrap):
    def columns(k):
        return range(width) if wrap else range(k, width - k)

    def first(i, carry):
        for j in columns(1):
            mid, beside = neighbours(u, i, j, width, wrap)
            r = f[i, j] - ((6.0 + s[i, j]) * mid - beside)
            res[i, j] = r
            d0[i, j] = r * (1.0 / CENTRE)
        return carry

    def second(i, carry):
        for j in columns(2):
            mid, beside = neighbours(d0, i, j, width, wrap)
            r = res[i, j] - ((6.0 + s[i, j]) * mid - beside)
            res[i, j] = r
            d1[i, j] = (FACTOR1 * FACTOR0) * mid + (2.0 * FACTOR1 / HALF) * r
        return carry

    def third(i, carry):
        for j in columns(3):
            mid, beside = neighbours(d1, i, j, width, wrap)
            r = res[i, j] - ((6.0 + s[i, j]) * mid - beside)
            d2 = (FACTOR2 * FACTOR1) * mid + (2.0 * FACTOR2 / HALF) * r
            emit(i, j, u[i, j] + d0[i, j] + mid + d2)
        return carry

    lax.fori_loop(low + 1, low + 5 + rows, first, 0)
    lax.fori_loop(low + 2, low + 4 + rows, second, 0)
    lax.fori_loop(low + 3, low + 3 + rows, third, 0)


def prolong_cell(lines, index, blocks, guess, a, b):
    total = guess[a, b]
    for k in range(2):
        ri, ci = index(a, b, k)
        total = total + lax.dot_general(
            lines[ri, ci], blocks[a, b, k], (((1,), (1,)), ((), ())), preferred_element_type=F32
        )
    return total


VMEM = pl.BlockSpec(memory_space=pltpu.VMEM)
HBM = pl.BlockSpec(memory_space=pltpu.HBM)


def fetch(sems, *pairs):
    copies = [pltpu.make_async_copy(a, b, sems.at[n]) for n, (a, b) in enumerate(pairs)]
    for copy in copies:
        copy.start()
    return copies


def fetched(*arrays):
    return [pltpu.VMEM(x.shape, x.dtype) for x in arrays] + [pltpu.SemaphoreType.DMA((len(arrays) + 1,))]


def smem_last(*arrays):
    *first, sems = fetched(*arrays)
    return [*first[:-1], pltpu.SMEM(arrays[-1].shape, arrays[-1].dtype), sems]


def call(kernel, inputs, outs, scratch, flops, vmem=16, hbm=()):
    nbytes = sum(x.size * x.dtype.itemsize for x in inputs)
    specs = [HBM if n in hbm else VMEM for n in range(len(inputs))]
    return pl.pallas_call(
        kernel,
        out_shape=outs,
        in_specs=specs,
        out_specs=jax.tree.map(lambda _: VMEM, outs),
        scratch_shapes=scratch,
        compiler_params=pltpu.CompilerParams(vmem_limit_bytes=vmem << 20),
        cost_estimate=pl.CostEstimate(flops=flops, bytes_accessed=nbytes, transcendentals=0),
    )(*inputs)


def cells(rows, cols, dtype=F32):
    return pltpu.VMEM((rows, cols, R, L), dtype)


def shifts(rows, cols):
    return pltpu.VMEM((rows, cols, 1, L), F32)


def pack_kernel(source_fourth, guess_fourth, shift_fourth, shift_third, source_third, out, s4, s3, sems):
    pairs = [(shift_fourth, s4), (shift_third, s3), (source_fourth.at[0, 0], out.at[0:16]), (guess_fourth.at[0, 0], out.at[16:32])]
    for i in range(2):
        for j in range(2):
            at = 40 + (i * 2 + j) * R
            pairs.append((source_third.at[i, j], out.at[at : at + R]))
    copies = fetch(sems, *pairs)
    copies[0].wait()
    copies[1].wait()
    out[32:33, :] = s4[0]
    for i in range(2):
        out[33 + 2 * i : 35 + 2 * i, :] = s3[i]
    out[37:40, :] = jnp.zeros((3, L), F32)
    for copy in copies[2:]:
        copy.wait()


def fourth_kernel(pair, a, a3, b, b3, links_h, blocks_h, guess_h, out, start, u, f, s, res, d0, d1, lines, blocks, guess, links, sems):
    copies = fetch(sems, (blocks_h, blocks), (guess_h, guess), (links_h, links))
    gz, gy = lax.axis_index("gz"), lax.axis_index("gy")
    core = lax.rem(gz, 2)

    def place(ref, chip, first_bit):
        for slot in range(2):
            bit = first_bit if slot == 0 else 1 - first_bit
            row = chip * 2 + bit
            for k in range(4):
                col = lax.bitwise_xor(gy, k)
                f[row, col] = ref[slot, k, 0:16, :]
                u[row, col] = ref[slot, k, 16:32, :]
                s[row, col] = ref[slot, k, 32:33, :]

    place(pair, 2, core)
    place(a, 1 + 2 * core, 1 - core)
    place(b, 3 - 2 * core, core)
    place(a3, 4 * core, 1 - core)
    place(b3, 4 - 4 * core, core)

    def emit(i, j, value):
        lines[i - 3 - core, j] = value.astype(BF16)
        res[i, j] = value

    smooth(u, f, s, res, d0, d1, emit, core, 3, 4, True)
    out[0, 0] = res[4 + core, gy]

    for copy in copies:
        copy.wait()

    def index(i, j, k):
        q = links[i, k, j]
        return lax.rem(q // 4 - gz + 1 + NZ, NZ), lax.rem(q, 4)

    for i in range(2):
        for j in range(2):
            start[i, j] = prolong_cell(lines, index, blocks, guess, i, j)


def third_kernel(pair, a, b, fpair, fa, fb, spair, sa, sb, links_h, blocks, guess_h, out, start, u, f, s, res, d0, d1, lines, guess, links, sems):
    copies = fetch(sems, (guess_h, guess), (links_h, links))
    gz, gy = lax.axis_index("gz"), lax.axis_index("gy")
    core = lax.rem(gz, 2)

    def place(ref, fref, sref, chip, first_bit):
        for slot in range(2):
            bit = first_bit if slot == 0 else 1 - first_bit
            for k in range(4):
                col = lax.bitwise_xor(gy, k) * 2
                for i in range(2):
                    row = chip * 4 + bit * 2 + i
                    for j in range(2):
                        at = (i * 2 + j) * R
                        u[row, col + j] = ref[slot, k, at : at + R, :]
                        f[row, col + j] = fref[slot, k, at : at + R, :]
                        s[row, col + j] = sref[slot, k, 33 + i * 2 + j : 34 + i * 2 + j, :]

    place(pair, fpair, spair, 1, core)
    place(a, fa, sa, 2 * core, 1 - core)
    place(b, fb, sb, 2 - 2 * core, core)

    def emit(i, j, value):
        lines[i - 3 - 2 * core, j] = value.astype(BF16)
        res[i, j] = value

    smooth(u, f, s, res, d0, d1, emit, 2 * core, 4, 8, True)
    for i in range(2):
        for j in range(2):
            out[i, j] = res[4 + 2 * core + i, 2 * gy + j]

    for copy in copies:
        copy.wait()

    def index(i, j, k):
        q = links[i, k, j]
        return lax.rem(q // 8 - 2 * gz + 1 + 2 * NZ, 2 * NZ), lax.rem(q, 8)

    for i in range(4):
        for j in range(4):
            start[i, j] = prolong_cell(lines, index, blocks, guess, i, j)


ALONG_Y, ALONG_Z = 544, 1224


def along_y_kernel(source_first, shift_first, source_second_h, shift_second_h, own, even, odd, source_second, shift_second, sems):
    copies = fetch(sems, (source_second_h, source_second), (shift_second_h, shift_second))
    side = lax.rem(lax.axis_index("gy"), 2)
    for copy in copies:
        copy.wait()
    for i in range(4):
        for j in range(4):
            at = (i * 4 + j) * R
            own[at : at + R, :] = source_second[i, j]
        own[256 + i * 4 : 260 + i * 4, :] = shift_second[i]
    for ref, first in ((even, 6 - 6 * side), (odd, 6 * side)):
        ref[0:272, :] = own[...]
        for i in range(8):
            for j in range(2):
                at = 272 + (i * 2 + j) * R
                ref[at : at + R, :] = source_first[i, first + j]
            ref[528 + i * 2 : 530 + i * 2, :] = jnp.where(first == 0, shift_first[i, 0:2, :], shift_first[i, 6:8, :])


def along_z_kernel(source_first, shift_first, own, even, odd, on, off):
    core = lax.rem(lax.axis_index("gz"), 2)
    for ref, first in ((on, 6 - 6 * core), (off, 6 * core)):
        ref[0:272, :] = own[...]
        ref[272:544, :] = even[0:272, :]
        ref[544:816, :] = odd[0:272, :]
        for i in range(2):
            row = first + i
            for j in range(8):
                at = 816 + (i * 12 + j) * R
                ref[at : at + R, :] = source_first[row, j]
            ref[1200 + i * 12 : 1208 + i * 12, :] = shift_first[row]
            for n, side_ref in enumerate((even, odd)):
                at = 816 + (i * 12 + 8 + 2 * n) * R
                ref[at : at + 2 * R, :] = side_ref[pl.ds(pl.multiple_of(272 + row * 2 * R, 8), 2 * R), :]
                low = side_ref[528 + 2 * i : 530 + 2 * i, :]
                high = side_ref[540 + 2 * i : 542 + 2 * i, :]
                ref[1208 + i * 12 + 2 * n : 1210 + i * 12 + 2 * n, :] = jnp.where(first == 0, low, high)


def second_kernel(own, own_even, own_odd, on, off, fown, feven, fodd, fon, foff, links_h, blocks, guess, out, start, even, odd, u, f, s, res, d0, d1, lines, links, sems):
    copies = fetch(sems, (links_h, links))
    gz, gy = lax.axis_index("gz"), lax.axis_index("gy")
    core, side = lax.rem(gz, 2), lax.rem(gy, 2)
    starts = (4, 8 - 8 * side, 8 * side)

    def place(refs, frefs, row0):
        for k in range(3):
            ref, base = refs[k]
            fref, fbase = frefs[k]
            for i in range(4):
                for j in range(4):
                    c = i * 4 + j
                    row, col = row0 + i, starts[k] + j
                    u[row, col] = ref[base + c * R : base + (c + 1) * R, :]
                    f[row, col] = fref[fbase + c * R : fbase + (c + 1) * R, :]
                    s[row, col] = fref[fbase + 256 + c : fbase + 257 + c, :]

    place(((own, 0), (own_even, 0), (own_odd, 0)), ((fown, 0), (feven, 0), (fodd, 0)), 4)
    for ref, fref, row0 in ((on, fon, 8 - 8 * core), (off, foff, 8 * core)):
        place([(ref, 256 * k) for k in range(3)], [(fref, 272 * k) for k in range(3)], row0)

    def emit(i, j, value):
        lines[i - 3, j - 3] = value.astype(BF16)
        res[i, j] = value

    smooth(u, f, s, res, d0, d1, emit, 0, 6, 12, False)
    for i in range(4):
        for j in range(4):
            out[i, j] = res[4 + i, 4 + j]

    for copy in copies:
        copy.wait()

    def index(i, j, k):
        q = links[i, k, j]
        row = lax.rem(q // 16 - 4 * gz + 1 + 4 * NZ, 4 * NZ)
        return row, lax.rem(lax.rem(q, 16) - 4 * gy + 1 + 4 * NY, 4 * NY)

    def row_of_cells(i, carry):
        for j in range(8):
            start[i, j] = prolong_cell(lines, index, blocks, guess, i, j)
        return carry

    lax.fori_loop(0, 8, row_of_cells, 0)
    for i in range(8):
        for j in range(3):
            at = (i * 3 + j) * R
            even[at : at + R, :] = start[i, 5 - 5 * side + j]
            odd[at : at + R, :] = start[i, 5 * side + j]


def rows_kernel(start, even, odd, on, off):
    core = lax.rem(lax.axis_index("gz"), 2)
    for ref, first in ((on, 5 - 5 * core), (off, 5 * core)):
        for i in range(3):
            for j in range(8):
                at = (i * 14 + j) * R
                ref[at : at + R, :] = start[first + i, j]
            for n, side_ref in enumerate((even, odd)):
                at = (i * 14 + 8 + 3 * n) * R
                ref[at : at + 3 * R, :] = side_ref[pl.ds(pl.multiple_of((first + i) * 3 * R, 8), 3 * R), :]


def first_kernel(own, even, odd, on, off, fown, sown, feven, fodd, fon, foff, out, u, f, s, res, d0, d1):
    gz, gy = lax.axis_index("gz"), lax.axis_index("gy")
    core, side = lax.rem(gz, 2), lax.rem(gy, 2)
    even_u, odd_u = 11 - 11 * side, 11 * side
    even_f, odd_f = 11 - 10 * side, 1 + 10 * side

    for i in range(8):
        for j in range(8):
            u[3 + i, 3 + j] = own[i, j]
            f[3 + i, 3 + j] = fown[i, j]
            s[3 + i, 3 + j] = sown[i, j : j + 1, :]
        for j in range(3):
            at = (i * 3 + j) * R
            u[3 + i, even_u + j] = even[at : at + R, :]
            u[3 + i, odd_u + j] = odd[at : at + R, :]
        for j in range(2):
            c = i * 2 + j
            at = 272 + c * R
            f[3 + i, even_f + j] = feven[at : at + R, :]
            f[3 + i, odd_f + j] = fodd[at : at + R, :]
            s[3 + i, even_f + j] = feven[528 + c : 529 + c, :]
            s[3 + i, odd_f + j] = fodd[528 + c : 529 + c, :]

    def place(ref, fref, row_u, row_f):
        for i in range(3):
            for j in range(14):
                col = 3 + j if j < 8 else even_u + j - 8 if j < 11 else odd_u + j - 11
                at = (i * 14 + j) * R
                u[row_u + i, col] = ref[at : at + R, :]
        for i in range(2):
            for j in range(12):
                col = 3 + j if j < 8 else even_f + j - 8 if j < 10 else odd_f + j - 10
                c = i * 12 + j
                at = 816 + c * R
                f[row_f + i, col] = fref[at : at + R, :]
                s[row_f + i, col] = fref[1200 + c : 1201 + c, :]

    place(on, fon, 11 - 11 * core, 11 - 10 * core)
    place(off, foff, 11 * core, 1 + 10 * core)

    def emit(i, j, value):
        out[i - 3, j - 3] = value

    smooth(u, f, s, res, d0, d1, emit, 0, 8, 14, False)


def sds(*shape, dtype=F32):
    return jax.ShapeDtypeStruct(shape, dtype)


def after(x, *done):
    return lax.optimization_barrier((x, *done))[0]


def flat(x):
    return x.reshape(-1, L)


def shards(
    source_first, source_second, source_third, source_fourth,
    guess_first, guess_second, guess_third, guess_fourth,
    shift_first, shift_second, shift_third, shift_fourth,
    blocks_first, blocks_second, blocks_third,
    links_first, links_second, links_third,
):
    links_first, links_second, links_third = (x.transpose(0, 2, 1) for x in (links_first, links_second, links_third))

    (pack,) = call(pack_kernel, (source_fourth, guess_fourth, shift_fourth, shift_third, source_third), (sds(104, L),), [pltpu.VMEM((1, 1, L), F32), pltpu.VMEM((2, 2, L), F32), pltpu.SemaphoreType.DMA((8,))], 1000, 2, range(5))
    y1, y2, y3 = y_by(pack, 1), y_by(pack, 2), y_by(pack, 3)
    line = jnp.stack([pack, y1, y2, y3])
    line_on = z_on(line)
    pair = jnp.stack([line[:, :40], line_on[:, :40]])
    pair_f = jnp.stack([line[:, 40:], line_on[:, 40:]])
    near = z_off(pair)
    far = z_off3(pair)

    mine, ahead_even, ahead_odd = call(
        along_y_kernel,
        (source_first, shift_first, source_second, shift_second),
        (sds(272, L), sds(ALONG_Y, L), sds(ALONG_Y, L)),
        fetched(source_second, shift_second), 10000, 4, (2, 3),
    )
    ahead_even, ahead_odd = y_even(after(ahead_even, y1, y2, y3)), y_odd(after(ahead_odd, y1, y2, y3))
    ahead_on, ahead_off = call(
        along_z_kernel,
        (source_first, shift_first, mine, ahead_even, ahead_odd),
        (sds(ALONG_Z, L), sds(ALONG_Z, L)),
        [], 10000, 6,
    )

    near_b, far_b = z_on(near), z_on(far)
    near_f = z_off(after(pair_f, near, far))
    near_fb = z_on(near_f)
    ahead_on = z_on(after(ahead_on, near_b, far_b))
    ahead_off = z_off(after(ahead_off, near_b, far_b))

    def smoothing_scratch(rows, cols):
        return [cells(rows, cols), cells(rows, cols), shifts(rows, cols)] + [cells(rows, cols)] * 3

    out_fourth, start_third = call(
        fourth_kernel,
        (pair, near, far, near_b, far_b, links_third, blocks_third, guess_third),
        (sds(1, 1, R, L), sds(2, 2, R, L)),
        smoothing_scratch(10, 4) + [cells(3, 4, BF16)] + smem_last(blocks_third, guess_third, links_third),
        4_000_000, 6, (5, 6, 7),
    )

    own = flat(start_third)
    line3 = jnp.stack([own, y_by(own, 1), y_by(own, 2), y_by(own, 3)])
    pair3 = jnp.stack([line3, z_on(line3)])
    near3 = z_off(pair3)
    near3_b = z_on(near3)
    out_third, start_second = call(
        third_kernel,
        (pair3, near3, near3_b, pair_f, near_f, near_fb, pair, near, near_b, links_second, blocks_second, guess_second),
        (sds(2, 2, R, L), sds(4, 4, R, L)),
        smoothing_scratch(12, 8) + [cells(4, 8, BF16)] + smem_last(guess_second, links_second),
        8_000_000, 12, (9, 11),
    )

    own = flat(start_second)
    own_even, own_odd = y_even(own), y_odd(own)
    block = jnp.concatenate([own, own_even, own_odd])
    out_second, start_first, strip_even, strip_odd = call(
        second_kernel,
        (own, own_even, own_odd, z_on(block), z_off(block), mine, ahead_even, ahead_odd, ahead_on, ahead_off, links_first, blocks_first, guess_first),
        (sds(4, 4, R, L), sds(8, 8, R, L), sds(24 * R, L), sds(24 * R, L)),
        smoothing_scratch(12, 12) + [cells(6, 6, BF16)] + smem_last(links_first),
        16_000_000, 20, (10,),
    )

    u_even, u_odd = y_even(strip_even), y_odd(strip_odd)
    u_on, u_off = call(rows_kernel, (start_first, u_even, u_odd), (sds(42 * R, L), sds(42 * R, L)), [], 10000, 4)
    (out_first,) = call(
        first_kernel,
        (start_first, u_even, u_odd, z_on(u_on), z_off(u_off), source_first, shift_first, ahead_even, ahead_odd, ahead_on, ahead_off),
        (sds(8, 8, R, L),),
        smoothing_scratch(14, 14),
        16_000_000, 20,
    )
    return out_first, out_second, out_third, out_fourth


def solution(mesh):
    field = P("gz", "gy", None, None)
    line = P("gz", "gy", None)
    block = P("gz", "gy", None, None, None)

    return jax.shard_map(
        shards,
        mesh=mesh,
        in_specs=(field,) * 8 + (line,) * 4 + (block,) * 3 + (line,) * 3,
        out_specs=(field,) * 4,
        check_vma=False,
    )
```

```python
import jax
import jax.numpy as jnp
from jax import lax
from jax.experimental import pallas as pl
from jax.experimental.pallas import tpu as pltpu
from jax.sharding import PartitionSpec as P


UPPER = 14.0
LOWER = UPPER / 8.0
CENTRE = (UPPER + LOWER) / 2.0
HALF = (UPPER - LOWER) / 2.0
RATIO = CENTRE / HALF
FACTOR0 = 1.0 / RATIO
FACTOR1 = 1.0 / (2.0 * RATIO - FACTOR0)
FACTOR2 = 1.0 / (2.0 * RATIO - FACTOR1)

F32 = jnp.float32
BF16 = jnp.bfloat16
R = 16
L = 128

NZ, NY = 64, 4


def swap(x, axis, partner):
    return lax.ppermute(x, axis, [(i, partner(i)) for i in range(lax.axis_size(axis))])


def z_on(x):
    return swap(x, "gz", lambda i: i ^ 1)


def z_off(x):
    return swap(x, "gz", lambda i: (((i + 1) ^ 1) - 1) % NZ)


def z_off3(x):
    return swap(x, "gz", lambda i: (i - 3 if i % 2 == 0 else i + 3) % NZ)


def y_by(x, k):
    return swap(x, "gy", lambda j: j ^ k)


def y_even(x):
    return y_by(x, 1)


def y_odd(x):
    return y_by(x, 3)


def neighbours(v, i, j, width, wrap):
    jl = (j - 1) % width if wrap else j - 1
    jr = (j + 1) % width if wrap else j + 1
    mid = v[i, j]
    beside = v[i - 1, j] + v[i + 1, j] + v[i, jl] + v[i, jr]
    beside = beside + pltpu.roll(mid, 1, 1) + pltpu.roll(mid, L - 1, 1)
    return mid, beside


def smooth(u, f, s, res, d0, d1, emit, low, rows, width, wrap):
    def columns(k):
        return range(width) if wrap else range(k, width - k)

    def first(i, carry):
        for j in columns(1):
            mid, beside = neighbours(u, i, j, width, wrap)
            r = f[i, j] - ((6.0 + s[i, j]) * mid - beside)
            res[i, j] = r
            d0[i, j] = r * (1.0 / CENTRE)
        return carry

    def second(i, carry):
        for j in columns(2):
            mid, beside = neighbours(d0, i, j, width, wrap)
            r = res[i, j] - ((6.0 + s[i, j]) * mid - beside)
            res[i, j] = r
            d1[i, j] = (FACTOR1 * FACTOR0) * mid + (2.0 * FACTOR1 / HALF) * r
        return carry

    def third(i, carry):
        for j in columns(3):
            mid, beside = neighbours(d1, i, j, width, wrap)
            r = res[i, j] - ((6.0 + s[i, j]) * mid - beside)
            d2 = (FACTOR2 * FACTOR1) * mid + (2.0 * FACTOR2 / HALF) * r
            emit(i, j, u[i, j] + d0[i, j] + mid + d2)
        return carry

    lax.fori_loop(low + 1, low + 5 + rows, first, 0)
    lax.fori_loop(low + 2, low + 4 + rows, second, 0)
    lax.fori_loop(low + 3, low + 3 + rows, third, 0)


def prolong_cell(lines, index, blocks, guess, a, b):
    total = guess[a, b]
    for k in range(2):
        ri, ci = index(a, b, k)
        total = total + lax.dot_general(
            lines[ri, ci], blocks[a, b, k], (((1,), (1,)), ((), ())), preferred_element_type=F32
        )
    return total


VMEM = pl.BlockSpec(memory_space=pltpu.VMEM)
HBM = pl.BlockSpec(memory_space=pltpu.HBM)


def fetch(sems, *pairs):
    copies = [pltpu.make_async_copy(a, b, sems.at[n]) for n, (a, b) in enumerate(pairs)]
    for copy in copies:
        copy.start()
    return copies


def fetched(*arrays):
    return [pltpu.VMEM(x.shape, x.dtype) for x in arrays] + [pltpu.SemaphoreType.DMA((len(arrays) + 1,))]


def smem_last(*arrays):
    *first, sems = fetched(*arrays)
    return [*first[:-1], pltpu.SMEM(arrays[-1].shape, arrays[-1].dtype), sems]


def call(kernel, inputs, outs, scratch, flops, vmem=16, hbm=()):
    nbytes = sum(x.size * x.dtype.itemsize for x in inputs)
    specs = [HBM if n in hbm else VMEM for n in range(len(inputs))]
    inputs = [pltpu.with_memory_space_constraint(x, pltpu.HBM) if n in hbm else x for n, x in enumerate(inputs)]
    return pl.pallas_call(
        kernel,
        out_shape=outs,
        in_specs=specs,
        out_specs=jax.tree.map(lambda _: VMEM, outs),
        scratch_shapes=scratch,
        compiler_params=pltpu.CompilerParams(vmem_limit_bytes=vmem << 20),
        cost_estimate=pl.CostEstimate(flops=flops, bytes_accessed=nbytes, transcendentals=0),
    )(*inputs)


def cells(rows, cols, dtype=F32):
    return pltpu.VMEM((rows, cols, R, L), dtype)


def shifts(rows, cols):
    return pltpu.VMEM((rows, cols, 1, L), F32)


def pack_kernel(source_fourth, guess_fourth, shift_fourth, shift_third, source_third, out, s4, s3, sems):
    pairs = [(shift_fourth, s4), (shift_third, s3), (source_fourth.at[0, 0], out.at[0:16]), (guess_fourth.at[0, 0], out.at[16:32])]
    for i in range(2):
        for j in range(2):
            at = 40 + (i * 2 + j) * R
            pairs.append((source_third.at[i, j], out.at[at : at + R]))
    copies = fetch(sems, *pairs)
    copies[0].wait()
    copies[1].wait()
    out[32:33, :] = s4[0]
    for i in range(2):
        out[33 + 2 * i : 35 + 2 * i, :] = s3[i]
    out[37:40, :] = jnp.zeros((3, L), F32)
    for copy in copies[2:]:
        copy.wait()


THIRD = 1232


def ahead_kernel(
    source_first_h, shift_first_h, source_second_h, shift_second_h, blocks_third, guess_third_h, links_third,
    third, own, even, odd, row_on, row_off,
    source_first, shift_first, source_second, shift_second, guess_third, links, sems,
):
    pairs = [
        (links_third, links), (guess_third_h, guess_third), (source_second_h, source_second), (shift_second_h, shift_second),
        (shift_first_h, shift_first), (source_first_h, source_first),
    ]
    for c in range(8):
        pairs.append((blocks_third.at[c // 4, c // 2 % 2, c % 2], third.at[c * L : (c + 1) * L]))
    copies = fetch(sems, *pairs)
    for copy in copies[:6]:
        copy.wait()
    for i in range(2):
        for j in range(2):
            rest = guess_third[i, j]
            for n in range(3):
                term = rest.astype(BF16)
                at = 1024 + n * 64 + (i * 2 + j) * R
                third[at : at + R, :] = term
                rest = rest - term.astype(F32)
    names = lax.broadcasted_iota(jnp.int32, (16, L), 0)
    rows = jnp.zeros((16, L), jnp.int32)
    for c in range(8):
        rows = jnp.where(names == c, links[c // 4, c // 2 % 2, c % 2], rows)
    third[1216:1232, :] = rows.astype(F32).astype(BF16)

    side, core = lax.rem(lax.axis_index("gy"), 2), lax.rem(lax.axis_index("gz"), 2)
    for i in range(4):
        for j in range(4):
            at = (i * 4 + j) * R
            own[at : at + R, :] = source_second[i, j]
        own[256 + i * 4 : 260 + i * 4, :] = shift_second[i]
    for ref, first in ((even, 6 - 6 * side), (odd, 6 * side)):
        ref[0:272, :] = own[...]
        for i in range(8):
            for j in range(2):
                at = 272 + (i * 2 + j) * R
                ref[at : at + R, :] = source_first[i, first + j]
            ref[528 + i * 2 : 530 + i * 2, :] = jnp.where(first == 0, shift_first[i, 0:2, :], shift_first[i, 6:8, :])
    for ref, first in ((row_on, 6 - 6 * core), (row_off, 6 * core)):
        for i in range(2):
            for j in range(8):
                at = (i * 8 + j) * R
                ref[at : at + R, :] = source_first[first + i, j]
            ref[256 + i * 8 : 264 + i * 8, :] = shift_first[first + i]
    for copy in copies[6:]:
        copy.wait()


def fourth_kernel(pair, a, a3, b, b3, third0, third1, third2, third3, out, start, u, f, s, res, d0, d1, lines):
    gz, gy = lax.axis_index("gz"), lax.axis_index("gy")
    core = lax.rem(gz, 2)

    def place(ref, chip, first_bit):
        for slot in range(2):
            bit = first_bit if slot == 0 else 1 - first_bit
            row = chip * 2 + bit
            for k in range(4):
                col = lax.bitwise_xor(gy, k)
                f[row, col] = ref[slot, k, 0:16, :]
                u[row, col] = ref[slot, k, 16:32, :]
                s[row, col] = ref[slot, k, 32:33, :]

    place(pair, 2, core)
    place(a, 1 + 2 * core, 1 - core)
    place(b, 3 - 2 * core, core)
    place(a3, 4 * core, 1 - core)
    place(b3, 4 - 4 * core, core)

    def emit(i, j, value):
        lines[i - 3 - core, j] = value.astype(BF16).astype(F32)
        res[i, j] = value

    smooth(u, f, s, res, d0, d1, emit, core, 3, 4, True)
    out[0, 0] = res[4 + core, gy]

    for n, ref in enumerate((third0, third1, third2, third3)):
        col = lax.bitwise_xor(gy, n) * 2
        for c in range(4):
            i, j = c // 2, c % 2
            at = 1024 + c * R
            total = (ref[at : at + R, :].astype(F32) + ref[at + 64 : at + 64 + R, :].astype(F32)) + ref[at + 128 : at + 128 + R, :].astype(F32)
            names = ref[1216:1232, :].astype(F32)
            for k in range(2):
                name = names[c * 2 + k : c * 2 + k + 1, :]
                line = jnp.zeros((R, L), F32)
                for row in range(3):
                    base = (lax.rem(gz + row - 1 + NZ, NZ) * 4).astype(F32)
                    for x in range(4):
                        line = jnp.where(jnp.broadcast_to(name == base + x, (R, L)), lines[row, x], line)
                at = (c * 2 + k) * L
                total = total + lax.dot_general(
                    line.astype(BF16), ref[at : at + L, :], (((1,), (1,)), ((), ())), preferred_element_type=F32
                )
            start[pl.ds(pl.multiple_of((i * 8 + col + j) * R, R), R), :] = total


def third_kernel(pair, a, b, fpair, fa, fb, spair, sa, sb, links_h, blocks, guess_h, out, start, u, f, s, res, d0, d1, lines, guess, links, sems):
    copies = fetch(sems, (guess_h, guess), (links_h, links))
    gz, gy = lax.axis_index("gz"), lax.axis_index("gy")
    core = lax.rem(gz, 2)

    def place(ref, fref, sref, chip, first_bit):
        for slot in range(2):
            bit = first_bit if slot == 0 else 1 - first_bit
            for k in range(4):
                col = lax.bitwise_xor(gy, k) * 2
                for i in range(2):
                    row = chip * 4 + bit * 2 + i
                    for j in range(2):
                        at = (i * 2 + j) * R
                        f[row, col + j] = fref[slot, k, at : at + R, :]
                        s[row, col + j] = sref[slot, k, 33 + i * 2 + j : 34 + i * 2 + j, :]
            for i in range(2):
                for j in range(8):
                    at = (i * 8 + j) * R
                    u[chip * 4 + bit * 2 + i, j] = ref[slot, at : at + R, :]

    place(pair, fpair, spair, 1, core)
    place(a, fa, sa, 2 * core, 1 - core)
    place(b, fb, sb, 2 - 2 * core, core)

    def emit(i, j, value):
        lines[i - 3 - 2 * core, j] = value.astype(BF16)
        res[i, j] = value

    smooth(u, f, s, res, d0, d1, emit, 2 * core, 4, 8, True)
    for i in range(2):
        for j in range(2):
            out[i, j] = res[4 + 2 * core + i, 2 * gy + j]

    for copy in copies:
        copy.wait()

    def index(i, j, k):
        q = links[i, k, j]
        return lax.rem(q // 8 - 2 * gz + 1 + 2 * NZ, 2 * NZ), lax.rem(q, 8)

    for i in range(4):
        for j in range(4):
            start[i, j] = prolong_cell(lines, index, blocks, guess, i, j)


ALONG_Y, ALONG_Z = 544, 1224


def along_z_kernel(own, even, odd, row_on, row_off, on, off):
    core = lax.rem(lax.axis_index("gz"), 2)
    for ref, rows, first in ((on, row_on, 6 - 6 * core), (off, row_off, 6 * core)):
        ref[0:272, :] = own[...]
        ref[272:544, :] = even[0:272, :]
        ref[544:816, :] = odd[0:272, :]
        for i in range(2):
            row = first + i
            at = 816 + i * 12 * R
            ref[at : at + 8 * R, :] = rows[i * 8 * R : (i + 1) * 8 * R, :]
            ref[1200 + i * 12 : 1208 + i * 12, :] = rows[256 + i * 8 : 264 + i * 8, :]
            for n, side_ref in enumerate((even, odd)):
                at = 816 + (i * 12 + 8 + 2 * n) * R
                ref[at : at + 2 * R, :] = side_ref[pl.ds(pl.multiple_of(272 + row * 2 * R, 8), 2 * R), :]
                low = side_ref[528 + 2 * i : 530 + 2 * i, :]
                high = side_ref[540 + 2 * i : 542 + 2 * i, :]
                ref[1208 + i * 12 + 2 * n : 1210 + i * 12 + 2 * n, :] = jnp.where(first == 0, low, high)


def second_kernel(own, own_even, own_odd, on, off, fown, feven, fodd, fon, foff, links_h, blocks, guess, out, start, even, odd, u, f, s, res, d0, d1, lines, links, sems):
    copies = fetch(sems, (links_h, links))
    gz, gy = lax.axis_index("gz"), lax.axis_index("gy")
    core, side = lax.rem(gz, 2), lax.rem(gy, 2)
    starts = (4, 8 - 8 * side, 8 * side)

    def place(refs, frefs, row0):
        for k in range(3):
            ref, base = refs[k]
            fref, fbase = frefs[k]
            for i in range(4):
                for j in range(4):
                    c = i * 4 + j
                    row, col = row0 + i, starts[k] + j
                    u[row, col] = ref[base + c * R : base + (c + 1) * R, :]
                    f[row, col] = fref[fbase + c * R : fbase + (c + 1) * R, :]
                    s[row, col] = fref[fbase + 256 + c : fbase + 257 + c, :]

    place(((own, 0), (own_even, 0), (own_odd, 0)), ((fown, 0), (feven, 0), (fodd, 0)), 4)
    for ref, fref, row0 in ((on, fon, 8 - 8 * core), (off, foff, 8 * core)):
        place([(ref, 256 * k) for k in range(3)], [(fref, 272 * k) for k in range(3)], row0)

    def emit(i, j, value):
        lines[i - 3, j - 3] = value.astype(BF16)
        res[i, j] = value

    smooth(u, f, s, res, d0, d1, emit, 0, 6, 12, False)
    for i in range(4):
        for j in range(4):
            out[i, j] = res[4 + i, 4 + j]

    for copy in copies:
        copy.wait()

    def index(i, j, k):
        q = links[i, k, j]
        row = lax.rem(q // 16 - 4 * gz + 1 + 4 * NZ, 4 * NZ)
        return row, lax.rem(lax.rem(q, 16) - 4 * gy + 1 + 4 * NY, 4 * NY)

    def row_of_cells(i, carry):
        for j in range(8):
            start[i, j] = prolong_cell(lines, index, blocks, guess, i, j)
        return carry

    lax.fori_loop(0, 8, row_of_cells, 0)
    for i in range(8):
        for j in range(3):
            at = (i * 3 + j) * R
            even[at : at + R, :] = start[i, 5 - 5 * side + j]
            odd[at : at + R, :] = start[i, 5 * side + j]


def rows_kernel(start, even, odd, on, off):
    core = lax.rem(lax.axis_index("gz"), 2)
    for ref, first in ((on, 5 - 5 * core), (off, 5 * core)):
        for i in range(3):
            for j in range(8):
                at = (i * 14 + j) * R
                ref[at : at + R, :] = start[first + i, j]
            for n, side_ref in enumerate((even, odd)):
                at = (i * 14 + 8 + 3 * n) * R
                ref[at : at + 3 * R, :] = side_ref[pl.ds(pl.multiple_of((first + i) * 3 * R, 8), 3 * R), :]


def first_kernel(own, even, odd, on, off, fown, sown, feven, fodd, fon, foff, out, u, f, s, res, d0, d1):
    gz, gy = lax.axis_index("gz"), lax.axis_index("gy")
    core, side = lax.rem(gz, 2), lax.rem(gy, 2)
    even_u, odd_u = 11 - 11 * side, 11 * side
    even_f, odd_f = 11 - 10 * side, 1 + 10 * side

    for i in range(8):
        for j in range(8):
            u[3 + i, 3 + j] = own[i, j]
            f[3 + i, 3 + j] = fown[i, j]
            s[3 + i, 3 + j] = sown[i, j : j + 1, :]
        for j in range(3):
            at = (i * 3 + j) * R
            u[3 + i, even_u + j] = even[at : at + R, :]
            u[3 + i, odd_u + j] = odd[at : at + R, :]
        for j in range(2):
            c = i * 2 + j
            at = 272 + c * R
            f[3 + i, even_f + j] = feven[at : at + R, :]
            f[3 + i, odd_f + j] = fodd[at : at + R, :]
            s[3 + i, even_f + j] = feven[528 + c : 529 + c, :]
            s[3 + i, odd_f + j] = fodd[528 + c : 529 + c, :]

    def place(ref, fref, row_u, row_f):
        for i in range(3):
            for j in range(14):
                col = 3 + j if j < 8 else even_u + j - 8 if j < 11 else odd_u + j - 11
                at = (i * 14 + j) * R
                u[row_u + i, col] = ref[at : at + R, :]
        for i in range(2):
            for j in range(12):
                col = 3 + j if j < 8 else even_f + j - 8 if j < 10 else odd_f + j - 10
                c = i * 12 + j
                at = 816 + c * R
                f[row_f + i, col] = fref[at : at + R, :]
                s[row_f + i, col] = fref[1200 + c : 1201 + c, :]

    place(on, fon, 11 - 11 * core, 11 - 10 * core)
    place(off, foff, 11 * core, 1 + 10 * core)

    def emit(i, j, value):
        out[i - 3, j - 3] = value

    smooth(u, f, s, res, d0, d1, emit, 0, 8, 14, False)


def sds(*shape, dtype=F32):
    return jax.ShapeDtypeStruct(shape, dtype)


def after(x, *done):
    return lax.optimization_barrier((x, *done))[0]


def flat(x):
    return x.reshape(-1, L)


def shards(
    source_first, source_second, source_third, source_fourth,
    guess_first, guess_second, guess_third, guess_fourth,
    shift_first, shift_second, shift_third, shift_fourth,
    blocks_first, blocks_second, blocks_third,
    links_first, links_second, links_third,
):
    links_first, links_second = links_first.transpose(0, 2, 1), links_second.transpose(0, 2, 1)

    (pack,) = call(
        pack_kernel,
        (source_fourth, guess_fourth, shift_fourth, shift_third, source_third),
        (sds(104, L),),
        [pltpu.VMEM((1, 1, L), F32), pltpu.VMEM((2, 2, L), F32), pltpu.SemaphoreType.DMA((8,))],
        1000, 2, range(5),
    )
    y1 = y_by(pack, 1)
    y2 = y_by(pack, 2)
    y3 = y_by(pack, 3)
    line = jnp.stack([pack, y1, y2, y3])
    line_on = z_on(line)
    pair = jnp.stack([line[:, :40], line_on[:, :40]])
    pair_f = jnp.stack([line[:, 40:], line_on[:, 40:]])
    near = z_off(pair)
    far = z_off3(pair)
    near_b = z_on(near)
    far_b = z_on(far)
    near_f = z_off(pair_f)
    near_fb = z_on(near_f)

    third, mine, ahead_even, ahead_odd, row_on, row_off = call(
        ahead_kernel,
        (source_first, shift_first, source_second, shift_second, blocks_third, guess_third, links_third),
        (sds(THIRD, L, dtype=BF16), sds(272, L), sds(ALONG_Y, L), sds(ALONG_Y, L), sds(272, L), sds(272, L)),
        [pltpu.VMEM(x.shape, x.dtype) for x in (source_first, shift_first, source_second, shift_second, guess_third)]
        + [pltpu.SMEM(links_third.shape, jnp.int32), pltpu.SemaphoreType.DMA((16,))],
        1000, 6, range(7),
    )
    third1 = y_by(third, 1)
    third2 = y_by(third, 2)
    third3 = y_by(third, 3)
    ahead_even, ahead_odd = y_even(after(ahead_even, y1, y2, y3)), y_odd(after(ahead_odd, y1, y2, y3))
    ahead_on, ahead_off = call(
        along_z_kernel,
        (mine, ahead_even, ahead_odd, row_on, row_off),
        (sds(ALONG_Z, L), sds(ALONG_Z, L)),
        [], 10000, 6,
    )
    ahead_on = z_on(ahead_on)
    ahead_off = z_off(ahead_off)

    def smoothing_scratch(rows, cols):
        return [cells(rows, cols), cells(rows, cols), shifts(rows, cols)] + [cells(rows, cols)] * 3

    out_fourth, start_third = call(
        fourth_kernel,
        (pair, near, far, near_b, far_b, third, third1, third2, third3),
        (sds(1, 1, R, L), sds(256, L)),
        smoothing_scratch(10, 4) + [cells(3, 4)],
        4_000_000, 6,
    )

    pair3 = jnp.stack([start_third, z_on(start_third)])
    near3 = z_off(pair3)
    near3_b = z_on(near3)
    out_third, start_second = call(
        third_kernel,
        (pair3, near3, near3_b, pair_f, near_f, near_fb, pair, near, near_b, links_second, blocks_second, guess_second),
        (sds(2, 2, R, L), sds(4, 4, R, L)),
        smoothing_scratch(12, 8) + [cells(4, 8, BF16)] + smem_last(guess_second, links_second),
        8_000_000, 12, (9, 11),
    )

    own = flat(start_second)
    own_even, own_odd = y_even(own), y_odd(own)
    block = jnp.concatenate([own, own_even, own_odd])
    out_second, start_first, strip_even, strip_odd = call(
        second_kernel,
        (own, own_even, own_odd, z_on(block), z_off(block), mine, ahead_even, ahead_odd, ahead_on, ahead_off, links_first, blocks_first, guess_first),
        (sds(4, 4, R, L), sds(8, 8, R, L), sds(24 * R, L), sds(24 * R, L)),
        smoothing_scratch(12, 12) + [cells(6, 6, BF16)] + smem_last(links_first),
        16_000_000, 20, (10,),
    )

    u_even, u_odd = y_even(strip_even), y_odd(strip_odd)
    u_on, u_off = call(rows_kernel, (start_first, u_even, u_odd), (sds(42 * R, L), sds(42 * R, L)), [], 10000, 4)
    (out_first,) = call(
        first_kernel,
        (start_first, u_even, u_odd, z_on(u_on), z_off(u_off), source_first, shift_first, ahead_even, ahead_odd, ahead_on, ahead_off),
        (sds(8, 8, R, L),),
        smoothing_scratch(14, 14),
        16_000_000, 20,
    )
    return out_first, out_second, out_third, out_fourth


def solution(mesh):
    field = P("gz", "gy", None, None)
    line = P("gz", "gy", None)
    block = P("gz", "gy", None, None, None)

    return jax.shard_map(
        shards,
        mesh=mesh,
        in_specs=(field,) * 8 + (line,) * 4 + (block,) * 3 + (line,) * 3,
        out_specs=(field,) * 4,
        check_vma=False,
    )
```

```python
import jax
import jax.numpy as jnp
from jax import lax
from jax.experimental import pallas as pl
from jax.experimental.pallas import tpu as pltpu
from jax.sharding import PartitionSpec as P


UPPER = 14.0
LOWER = UPPER / 8.0
CENTRE = (UPPER + LOWER) / 2.0
HALF = (UPPER - LOWER) / 2.0
RATIO = CENTRE / HALF
FACTOR0 = 1.0 / RATIO
FACTOR1 = 1.0 / (2.0 * RATIO - FACTOR0)
FACTOR2 = 1.0 / (2.0 * RATIO - FACTOR1)

F32 = jnp.float32
BF16 = jnp.bfloat16
R = 16
L = 128

NZ, NY = 64, 4


def swap(x, axis, partner):
    return lax.ppermute(x, axis, [(i, partner(i)) for i in range(lax.axis_size(axis))])


def z_on(x):
    return swap(x, "gz", lambda i: i ^ 1)


def z_off(x):
    return swap(x, "gz", lambda i: (((i + 1) ^ 1) - 1) % NZ)


def z_off3(x):
    return swap(x, "gz", lambda i: (i - 3 if i % 2 == 0 else i + 3) % NZ)


def y_by(x, k):
    return swap(x, "gy", lambda j: j ^ k)


def y_even(x):
    return y_by(x, 1)


def y_odd(x):
    return y_by(x, 3)


def neighbours(v, i, j, width, wrap):
    jl = (j - 1) % width if wrap else j - 1
    jr = (j + 1) % width if wrap else j + 1
    mid = v[i, j]
    beside = v[i - 1, j] + v[i + 1, j] + v[i, jl] + v[i, jr]
    beside = beside + pltpu.roll(mid, 1, 1) + pltpu.roll(mid, L - 1, 1)
    return mid, beside


def smooth(u, f, s, res, d0, d1, emit, low, rows, width, wrap):
    def columns(k):
        return range(width) if wrap else range(k, width - k)

    def first(i, carry):
        for j in columns(1):
            mid, beside = neighbours(u, i, j, width, wrap)
            r = f[i, j] - ((6.0 + s[i, j]) * mid - beside)
            res[i, j] = r
            d0[i, j] = r * (1.0 / CENTRE)
        return carry

    def second(i, carry):
        for j in columns(2):
            mid, beside = neighbours(d0, i, j, width, wrap)
            r = res[i, j] - ((6.0 + s[i, j]) * mid - beside)
            res[i, j] = r
            d1[i, j] = (FACTOR1 * FACTOR0) * mid + (2.0 * FACTOR1 / HALF) * r
        return carry

    def third(i, carry):
        for j in columns(3):
            mid, beside = neighbours(d1, i, j, width, wrap)
            r = res[i, j] - ((6.0 + s[i, j]) * mid - beside)
            d2 = (FACTOR2 * FACTOR1) * mid + (2.0 * FACTOR2 / HALF) * r
            emit(i, j, u[i, j] + d0[i, j] + mid + d2)
        return carry

    lax.fori_loop(low + 1, low + 5 + rows, first, 0)
    lax.fori_loop(low + 2, low + 4 + rows, second, 0)
    lax.fori_loop(low + 3, low + 3 + rows, third, 0)


def prolong_cell(lines, index, blocks, guess, a, b):
    total = guess[a, b]
    for k in range(2):
        ri, ci = index(a, b, k)
        total = total + lax.dot_general(
            lines[ri, ci], blocks[a, b, k], (((1,), (1,)), ((), ())), preferred_element_type=F32
        )
    return total


VMEM = pl.BlockSpec(memory_space=pltpu.VMEM)
HBM = pl.BlockSpec(memory_space=pltpu.HBM)


def fetch(sems, *pairs):
    copies = [pltpu.make_async_copy(a, b, sems.at[n]) for n, (a, b) in enumerate(pairs)]
    for copy in copies:
        copy.start()
    return copies


def fetched(*arrays):
    return [pltpu.VMEM(x.shape, x.dtype) for x in arrays] + [pltpu.SemaphoreType.DMA((len(arrays) + 1,))]


def smem_last(*arrays):
    *first, sems = fetched(*arrays)
    return [*first[:-1], pltpu.SMEM(arrays[-1].shape, arrays[-1].dtype), sems]


def call(kernel, inputs, outs, scratch, flops, vmem=16, hbm=()):
    nbytes = sum(x.size * x.dtype.itemsize for x in inputs)
    specs = [HBM if n in hbm else VMEM for n in range(len(inputs))]
    inputs = [pltpu.with_memory_space_constraint(x, pltpu.HBM) if n in hbm else x for n, x in enumerate(inputs)]
    return pl.pallas_call(
        kernel,
        out_shape=outs,
        in_specs=specs,
        out_specs=jax.tree.map(lambda _: VMEM, outs),
        scratch_shapes=scratch,
        compiler_params=pltpu.CompilerParams(vmem_limit_bytes=vmem << 20),
        cost_estimate=pl.CostEstimate(flops=flops, bytes_accessed=nbytes, transcendentals=0),
    )(*inputs)


def cells(rows, cols, dtype=F32):
    return pltpu.VMEM((rows, cols, R, L), dtype)


def shifts(rows, cols):
    return pltpu.VMEM((rows, cols, 1, L), F32)


def pack_kernel(source_fourth, guess_fourth, shift_fourth, shift_third, source_third, out, s4, s3, sems):
    pairs = [(shift_fourth, s4), (shift_third, s3), (source_fourth.at[0, 0], out.at[0:16]), (guess_fourth.at[0, 0], out.at[16:32])]
    for i in range(2):
        for j in range(2):
            at = 40 + (i * 2 + j) * R
            pairs.append((source_third.at[i, j], out.at[at : at + R]))
    copies = fetch(sems, *pairs)
    copies[0].wait()
    copies[1].wait()
    out[32:33, :] = s4[0]
    for i in range(2):
        out[33 + 2 * i : 35 + 2 * i, :] = s3[i]
    out[37:40, :] = jnp.zeros((3, L), F32)
    for copy in copies[2:]:
        copy.wait()


THIRD = 1232


def ahead_kernel(
    source_first_h, shift_first_h, source_second_h, shift_second_h, blocks_third, guess_third_h, links_third,
    third, own, even, odd, row_on, row_off,
    source_first, shift_first, source_second, shift_second, guess_third, links, sems,
):
    pairs = [
        (links_third, links), (guess_third_h, guess_third), (source_second_h, source_second), (shift_second_h, shift_second),
        (shift_first_h, shift_first), (source_first_h, source_first),
    ]
    for c in range(8):
        pairs.append((blocks_third.at[c // 4, c // 2 % 2, c % 2], third.at[c * L : (c + 1) * L]))
    copies = fetch(sems, *pairs)
    for copy in copies[:6]:
        copy.wait()
    for i in range(2):
        for j in range(2):
            rest = guess_third[i, j]
            for n in range(3):
                term = rest.astype(BF16)
                at = 1024 + n * 64 + (i * 2 + j) * R
                third[at : at + R, :] = term
                rest = rest - term.astype(F32)
    names = lax.broadcasted_iota(jnp.int32, (16, L), 0)
    rows = jnp.zeros((16, L), jnp.int32)
    for c in range(8):
        rows = jnp.where(names == c, links[c // 4, c // 2 % 2, c % 2], rows)
    third[1216:1232, :] = rows.astype(F32).astype(BF16)

    side, core = lax.rem(lax.axis_index("gy"), 2), lax.rem(lax.axis_index("gz"), 2)
    for i in range(4):
        for j in range(4):
            at = (i * 4 + j) * R
            own[at : at + R, :] = source_second[i, j]
        own[256 + i * 4 : 260 + i * 4, :] = shift_second[i]
    for ref, first in ((even, 6 - 6 * side), (odd, 6 * side)):
        ref[0:272, :] = own[...]
        for i in range(8):
            for j in range(2):
                at = 272 + (i * 2 + j) * R
                ref[at : at + R, :] = source_first[i, first + j]
            ref[528 + i * 2 : 530 + i * 2, :] = jnp.where(first == 0, shift_first[i, 0:2, :], shift_first[i, 6:8, :])
    for ref, first in ((row_on, 6 - 6 * core), (row_off, 6 * core)):
        for i in range(2):
            for j in range(8):
                at = (i * 8 + j) * R
                ref[at : at + R, :] = source_first[first + i, j]
            ref[256 + i * 8 : 264 + i * 8, :] = shift_first[first + i]
    for copy in copies[6:]:
        copy.wait()


def relay_kernel(near, far, out):
    out[0] = near[...]
    out[1] = far[...]


def fourth_kernel(pair, a, a3, both, third0, third1, third2, third3, out, start, u, f, s, res, d0, d1, lines):
    gz, gy = lax.axis_index("gz"), lax.axis_index("gy")
    core = lax.rem(gz, 2)

    def place(ref, chip, first_bit):
        for slot in range(2):
            bit = first_bit if slot == 0 else 1 - first_bit
            row = chip * 2 + bit
            for k in range(4):
                col = lax.bitwise_xor(gy, k)
                f[row, col] = ref[slot, k, 0:16, :]
                u[row, col] = ref[slot, k, 16:32, :]
                s[row, col] = ref[slot, k, 32:33, :]

    place(pair, 2, core)
    place(a, 1 + 2 * core, 1 - core)
    place(both.at[0], 3 - 2 * core, core)
    place(a3, 4 * core, 1 - core)
    place(both.at[1], 4 - 4 * core, core)

    def emit(i, j, value):
        lines[i - 3 - core, j] = value.astype(BF16).astype(F32)
        res[i, j] = value

    smooth(u, f, s, res, d0, d1, emit, core, 3, 4, True)
    out[0, 0] = res[4 + core, gy]

    for n, ref in enumerate((third0, third1, third2, third3)):
        col = lax.bitwise_xor(gy, n) * 2
        for c in range(4):
            i, j = c // 2, c % 2
            at = 1024 + c * R
            total = (ref[at : at + R, :].astype(F32) + ref[at + 64 : at + 64 + R, :].astype(F32)) + ref[at + 128 : at + 128 + R, :].astype(F32)
            names = ref[1216:1232, :].astype(F32)
            for k in range(2):
                name = names[c * 2 + k : c * 2 + k + 1, :]
                line = jnp.zeros((R, L), F32)
                for row in range(3):
                    base = (lax.rem(gz + row - 1 + NZ, NZ) * 4).astype(F32)
                    for x in range(4):
                        line = jnp.where(jnp.broadcast_to(name == base + x, (R, L)), lines[row, x], line)
                at = (c * 2 + k) * L
                total = total + lax.dot_general(
                    line.astype(BF16), ref[at : at + L, :], (((1,), (1,)), ((), ())), preferred_element_type=F32
                )
            start[pl.ds(pl.multiple_of((i * 8 + col + j) * R, R), R), :] = total


def third_kernel(pair, a, b, fpair, fa, fb, spair, sa, sb, links_h, blocks, guess_h, out, start, u, f, s, res, d0, d1, lines, guess, links, sems):
    copies = fetch(sems, (guess_h, guess), (links_h, links))
    gz, gy = lax.axis_index("gz"), lax.axis_index("gy")
    core = lax.rem(gz, 2)

    def place(ref, fref, sref, chip, first_bit):
        for slot in range(2):
            bit = first_bit if slot == 0 else 1 - first_bit
            for k in range(4):
                col = lax.bitwise_xor(gy, k) * 2
                for i in range(2):
                    row = chip * 4 + bit * 2 + i
                    for j in range(2):
                        at = (i * 2 + j) * R
                        f[row, col + j] = fref[slot, k, at : at + R, :]
                        s[row, col + j] = sref[slot, k, 33 + i * 2 + j : 34 + i * 2 + j, :]
            for i in range(2):
                for j in range(8):
                    at = (i * 8 + j) * R
                    u[chip * 4 + bit * 2 + i, j] = ref[slot, at : at + R, :]

    place(pair, fpair, spair, 1, core)
    place(a, fa, sa, 2 * core, 1 - core)
    place(b, fb, sb.at[0], 2 - 2 * core, core)

    def emit(i, j, value):
        lines[i - 3 - 2 * core, j] = value.astype(BF16)
        res[i, j] = value

    smooth(u, f, s, res, d0, d1, emit, 2 * core, 4, 8, True)
    for i in range(2):
        for j in range(2):
            out[i, j] = res[4 + 2 * core + i, 2 * gy + j]

    for copy in copies:
        copy.wait()

    def index(i, j, k):
        q = links[i, k, j]
        return lax.rem(q // 8 - 2 * gz + 1 + 2 * NZ, 2 * NZ), lax.rem(q, 8)

    for i in range(4):
        for j in range(4):
            start[i, j] = prolong_cell(lines, index, blocks, guess, i, j)


ALONG_Y, ALONG_Z = 544, 1224


def along_z_kernel(own, even, odd, row_on, row_off, on, off):
    core = lax.rem(lax.axis_index("gz"), 2)
    for ref, rows, first in ((on, row_on, 6 - 6 * core), (off, row_off, 6 * core)):
        ref[0:272, :] = own[...]
        ref[272:544, :] = even[0:272, :]
        ref[544:816, :] = odd[0:272, :]
        for i in range(2):
            row = first + i
            at = 816 + i * 12 * R
            ref[at : at + 8 * R, :] = rows[i * 8 * R : (i + 1) * 8 * R, :]
            ref[1200 + i * 12 : 1208 + i * 12, :] = rows[256 + i * 8 : 264 + i * 8, :]
            for n, side_ref in enumerate((even, odd)):
                at = 816 + (i * 12 + 8 + 2 * n) * R
                ref[at : at + 2 * R, :] = side_ref[pl.ds(pl.multiple_of(272 + row * 2 * R, 8), 2 * R), :]
                low = side_ref[528 + 2 * i : 530 + 2 * i, :]
                high = side_ref[540 + 2 * i : 542 + 2 * i, :]
                ref[1208 + i * 12 + 2 * n : 1210 + i * 12 + 2 * n, :] = jnp.where(first == 0, low, high)


SIDE4 = tuple((r, n) for r in range(4) for n in range(4 - r))
BLOCK = (16 + 2 * len(SIDE4)) * R


def at_cell(ref, cell):
    return ref[pl.ds(pl.multiple_of(cell * R, R), R), :]


def block_kernel(own, even, odd, on, off):
    core, side = lax.rem(lax.axis_index("gz"), 2), lax.rem(lax.axis_index("gy"), 2)
    for ref, right in ((on, 1 - core), (off, core)):
        for r in range(4):
            row = r + right * (3 - 2 * r)
            for j in range(4):
                at = (r * 4 + j) * R
                ref[at : at + R, :] = at_cell(own, row * 4 + j)
        for m, (r, n) in enumerate(SIDE4):
            row = r + right * (3 - 2 * r)
            for k, (beside, left) in enumerate(((even, side), (odd, 1 - side))):
                at = (16 + k * len(SIDE4) + m) * R
                ref[at : at + R, :] = at_cell(beside, row * 4 + n + left * (3 - 2 * n))


def second_kernel(own, own_even, own_odd, on, off, fown, feven, fodd, fon, foff, links_h, blocks, guess, out, start, even, odd, u, f, s, res, d0, d1, lines, links, sems):
    copies = fetch(sems, (links_h, links))
    gz, gy = lax.axis_index("gz"), lax.axis_index("gy")
    core, side = lax.rem(gz, 2), lax.rem(gy, 2)
    starts = (4, 8 - 8 * side, 8 * side)

    def place(frefs, row0):
        for k in range(3):
            fref, fbase = frefs[k]
            for i in range(4):
                for j in range(4):
                    c = i * 4 + j
                    row, col = row0 + i, starts[k] + j
                    f[row, col] = fref[fbase + c * R : fbase + (c + 1) * R, :]
                    s[row, col] = fref[fbase + 256 + c : fbase + 257 + c, :]

    place(((fown, 0), (feven, 0), (fodd, 0)), 4)
    for fref, row0 in ((fon, 8 - 8 * core), (foff, 8 * core)):
        place([(fref, 272 * k) for k in range(3)], row0)
    for i in range(4):
        for j in range(4):
            at = (i * 4 + j) * R
            for k, ref in enumerate((own, own_even, own_odd)):
                u[4 + i, starts[k] + j] = ref[at : at + R, :]
    for ref, left in ((on, core), (off, 1 - core)):
        for r in range(4):
            row = 8 + r - left * (5 + 2 * r)
            for j in range(4):
                at = (r * 4 + j) * R
                u[row, 4 + j] = ref[at : at + R, :]
        for m, (r, n) in enumerate(SIDE4):
            row = 8 + r - left * (5 + 2 * r)
            for k, across in enumerate((side, 1 - side)):
                at = (16 + k * len(SIDE4) + m) * R
                u[row, 8 + n - across * (5 + 2 * n)] = ref[at : at + R, :]

    def emit(i, j, value):
        lines[i - 3, j - 3] = value.astype(BF16)
        res[i, j] = value

    smooth(u, f, s, res, d0, d1, emit, 0, 6, 12, False)
    for i in range(4):
        for j in range(4):
            out[i, j] = res[4 + i, 4 + j]

    for copy in copies:
        copy.wait()

    def index(i, j, k):
        q = links[i, k, j]
        row = lax.rem(q // 16 - 4 * gz + 1 + 4 * NZ, 4 * NZ)
        return row, lax.rem(lax.rem(q, 16) - 4 * gy + 1 + 4 * NY, 4 * NY)

    def row_of_cells(i, carry):
        for j in range(8):
            start[i, j] = prolong_cell(lines, index, blocks, guess, i, j)
        return carry

    lax.fori_loop(0, 8, row_of_cells, 0)
    for i in range(8):
        for j in range(3):
            at = (i * 3 + j) * R
            even[at : at + R, :] = start[i, 5 - 5 * side + j]
            odd[at : at + R, :] = start[i, 5 * side + j]


SIDE3 = ((0, 0), (0, 1), (1, 0))
ROWS = (24 + 2 * len(SIDE3)) * R


def rows_kernel(start, even, odd, on, off):
    core, side = lax.rem(lax.axis_index("gz"), 2), lax.rem(lax.axis_index("gy"), 2)
    for ref, right in ((on, 1 - core), (off, core)):
        for r in range(3):
            row = r + right * (7 - 2 * r)
            for j in range(8):
                at = (r * 8 + j) * R
                ref[at : at + R, :] = start[row, j]
        for m, (r, n) in enumerate(SIDE3):
            row = r + right * (7 - 2 * r)
            for k, (beside, left) in enumerate(((even, side), (odd, 1 - side))):
                at = (24 + k * len(SIDE3) + m) * R
                ref[at : at + R, :] = at_cell(beside, row * 3 + n + left * (2 - 2 * n))


def first_kernel(own, even, odd, on, off, fown, sown, feven, fodd, fon, foff, out, u, f, s, res, d0, d1):
    gz, gy = lax.axis_index("gz"), lax.axis_index("gy")
    core, side = lax.rem(gz, 2), lax.rem(gy, 2)
    even_u, odd_u = 11 - 11 * side, 11 * side
    even_f, odd_f = 11 - 10 * side, 1 + 10 * side

    for i in range(8):
        for j in range(8):
            u[3 + i, 3 + j] = own[i, j]
            f[3 + i, 3 + j] = fown[i, j]
            s[3 + i, 3 + j] = sown[i, j : j + 1, :]
        for j in range(3):
            at = (i * 3 + j) * R
            u[3 + i, even_u + j] = even[at : at + R, :]
            u[3 + i, odd_u + j] = odd[at : at + R, :]
        for j in range(2):
            c = i * 2 + j
            at = 272 + c * R
            f[3 + i, even_f + j] = feven[at : at + R, :]
            f[3 + i, odd_f + j] = fodd[at : at + R, :]
            s[3 + i, even_f + j] = feven[528 + c : 529 + c, :]
            s[3 + i, odd_f + j] = fodd[528 + c : 529 + c, :]

    def place(ref, fref, left, row_f):
        for r in range(3):
            for j in range(8):
                at = (r * 8 + j) * R
                u[11 + r - left * (9 + 2 * r), 3 + j] = ref[at : at + R, :]
        for m, (r, n) in enumerate(SIDE3):
            for k, across in enumerate((side, 1 - side)):
                at = (24 + k * len(SIDE3) + m) * R
                u[11 + r - left * (9 + 2 * r), 11 + n - across * (9 + 2 * n)] = ref[at : at + R, :]
        for i in range(2):
            for j in range(12):
                col = 3 + j if j < 8 else even_f + j - 8 if j < 10 else odd_f + j - 10
                c = i * 12 + j
                at = 816 + c * R
                f[row_f + i, col] = fref[at : at + R, :]
                s[row_f + i, col] = fref[1200 + c : 1201 + c, :]

    place(on, fon, core, 11 - 10 * core)
    place(off, foff, 1 - core, 1 + 10 * core)

    def emit(i, j, value):
        out[i - 3, j - 3] = value

    smooth(u, f, s, res, d0, d1, emit, 0, 8, 14, False)


def sds(*shape, dtype=F32):
    return jax.ShapeDtypeStruct(shape, dtype)


def flat(x):
    return x.reshape(-1, L)


def shards(
    source_first, source_second, source_third, source_fourth,
    guess_first, guess_second, guess_third, guess_fourth,
    shift_first, shift_second, shift_third, shift_fourth,
    blocks_first, blocks_second, blocks_third,
    links_first, links_second, links_third,
):
    links_first, links_second = links_first.transpose(0, 2, 1), links_second.transpose(0, 2, 1)

    (pack,) = call(
        pack_kernel,
        (source_fourth, guess_fourth, shift_fourth, shift_third, source_third),
        (sds(104, L),),
        [pltpu.VMEM((1, 1, L), F32), pltpu.VMEM((2, 2, L), F32), pltpu.SemaphoreType.DMA((8,))],
        1000, 2, range(5),
    )
    y1 = y_by(pack, 1)
    y2 = y_by(pack, 2)
    y3 = y_by(pack, 3)
    line = jnp.stack([pack, y1, y2, y3])
    line_on = z_on(line)
    pair = jnp.stack([line[:, :40], line_on[:, :40]])
    pair_f = jnp.stack([line[:, 40:], line_on[:, 40:]])
    near = z_off(pair)
    far = z_off3(pair)
    (both,) = call(relay_kernel, (near, far), (sds(2, 2, 4, 40, L),), [], 1000, 2)
    both = z_on(both)
    near_f = z_off(pair_f)
    near_fb = z_on(near_f)

    third, mine, ahead_even, ahead_odd, row_on, row_off = call(
        ahead_kernel,
        (source_first, shift_first, source_second, shift_second, blocks_third, guess_third, links_third),
        (sds(THIRD, L, dtype=BF16), sds(272, L), sds(ALONG_Y, L), sds(ALONG_Y, L), sds(272, L), sds(272, L)),
        [pltpu.VMEM(x.shape, x.dtype) for x in (source_first, shift_first, source_second, shift_second, guess_third)]
        + [pltpu.SMEM(links_third.shape, jnp.int32), pltpu.SemaphoreType.DMA((16,))],
        1000, 6, range(7),
    )
    third1 = y_by(third, 1)
    third2 = y_by(third, 2)
    third3 = y_by(third, 3)
    ahead_even = y_even(ahead_even)
    ahead_odd = y_odd(ahead_odd)
    ahead_on, ahead_off = call(
        along_z_kernel,
        (mine, ahead_even, ahead_odd, row_on, row_off),
        (sds(ALONG_Z, L), sds(ALONG_Z, L)),
        [], 10000, 6,
    )
    ahead_on = z_on(ahead_on)
    ahead_off = z_off(ahead_off)

    def smoothing_scratch(rows, cols):
        return [cells(rows, cols), cells(rows, cols), shifts(rows, cols)] + [cells(rows, cols)] * 3

    out_fourth, start_third = call(
        fourth_kernel,
        (pair, near, far, both, third, third1, third2, third3),
        (sds(1, 1, R, L), sds(256, L)),
        smoothing_scratch(10, 4) + [cells(3, 4)],
        4_000_000, 6,
    )

    start_on = z_on(start_third)
    pair3 = jnp.stack([start_third, start_on])
    near3 = z_off(pair3)
    near3_b = z_on(near3)
    out_third, start_second = call(
        third_kernel,
        (pair3, near3, near3_b, pair_f, near_f, near_fb, pair, near, both, links_second, blocks_second, guess_second),
        (sds(2, 2, R, L), sds(4, 4, R, L)),
        smoothing_scratch(12, 8) + [cells(4, 8, BF16)] + smem_last(guess_second, links_second),
        8_000_000, 12, (9, 11),
    )

    own = flat(start_second)
    own_even, own_odd = y_even(own), y_odd(own)
    block_on, block_off = call(block_kernel, (own, own_even, own_odd), (sds(BLOCK, L), sds(BLOCK, L)), [], 10000, 4)
    out_second, start_first, strip_even, strip_odd = call(
        second_kernel,
        (own, own_even, own_odd, z_on(block_on), z_off(block_off), mine, ahead_even, ahead_odd, ahead_on, ahead_off, links_first, blocks_first, guess_first),
        (sds(4, 4, R, L), sds(8, 8, R, L), sds(24 * R, L), sds(24 * R, L)),
        smoothing_scratch(12, 12) + [cells(6, 6, BF16)] + smem_last(links_first),
        16_000_000, 20, (10,),
    )

    u_even, u_odd = y_even(strip_even), y_odd(strip_odd)
    u_on, u_off = call(rows_kernel, (start_first, u_even, u_odd), (sds(ROWS, L), sds(ROWS, L)), [], 10000, 4)
    (out_first,) = call(
        first_kernel,
        (start_first, u_even, u_odd, z_on(u_on), z_off(u_off), source_first, shift_first, ahead_even, ahead_odd, ahead_on, ahead_off),
        (sds(8, 8, R, L),),
        smoothing_scratch(14, 14),
        16_000_000, 20,
    )
    return out_first, out_second, out_third, out_fourth


def solution(mesh):
    field = P("gz", "gy", None, None)
    line = P("gz", "gy", None)
    block = P("gz", "gy", None, None, None)

    return jax.shard_map(
        shards,
        mesh=mesh,
        in_specs=(field,) * 8 + (line,) * 4 + (block,) * 3 + (line,) * 3,
        out_specs=(field,) * 4,
        check_vma=False,
    )
```

```python
import jax
import jax.numpy as jnp
from jax import lax
from jax.experimental import pallas as pl
from jax.experimental.pallas import tpu as pltpu
from jax.sharding import PartitionSpec as P


UPPER = 14.0
LOWER = UPPER / 8.0
CENTRE = (UPPER + LOWER) / 2.0
HALF = (UPPER - LOWER) / 2.0
RATIO = CENTRE / HALF
FACTOR0 = 1.0 / RATIO
FACTOR1 = 1.0 / (2.0 * RATIO - FACTOR0)
FACTOR2 = 1.0 / (2.0 * RATIO - FACTOR1)

F32 = jnp.float32
BF16 = jnp.bfloat16
R = 16
L = 128

NZ, NY = 64, 4


def swap(x, axis, partner):
    return lax.ppermute(x, axis, [(i, partner(i)) for i in range(lax.axis_size(axis))])


def z_on(x):
    return swap(x, "gz", lambda i: i ^ 1)


def z_off(x):
    return swap(x, "gz", lambda i: (((i + 1) ^ 1) - 1) % NZ)


def z_off3(x):
    return swap(x, "gz", lambda i: (i - 3 if i % 2 == 0 else i + 3) % NZ)


def y_by(x, k):
    return swap(x, "gy", lambda j: j ^ k)


def y_even(x):
    return y_by(x, 1)


def y_odd(x):
    return y_by(x, 3)


def neighbours(v, i, j, width, wrap):
    jl = (j - 1) % width if wrap else j - 1
    jr = (j + 1) % width if wrap else j + 1
    mid = v[i, j]
    beside = v[i - 1, j] + v[i + 1, j] + v[i, jl] + v[i, jr]
    beside = beside + pltpu.roll(mid, 1, 1) + pltpu.roll(mid, L - 1, 1)
    return mid, beside


def smooth(u, f, s, res, d0, d1, emit, low, rows, width, wrap, row_done=lambda i: None):
    def columns(k):
        return range(width) if wrap else range(k, width - k)

    def first(i, carry):
        for j in columns(1):
            mid, beside = neighbours(u, i, j, width, wrap)
            r = f[i, j] - ((6.0 + s[i, j]) * mid - beside)
            res[i, j] = r
            d0[i, j] = r * (1.0 / CENTRE)
        return carry

    def second(i, carry):
        for j in columns(2):
            mid, beside = neighbours(d0, i, j, width, wrap)
            r = res[i, j] - ((6.0 + s[i, j]) * mid - beside)
            res[i, j] = r
            d1[i, j] = (FACTOR1 * FACTOR0) * mid + (2.0 * FACTOR1 / HALF) * r
        return carry

    def third(i, carry):
        for j in columns(3):
            mid, beside = neighbours(d1, i, j, width, wrap)
            r = res[i, j] - ((6.0 + s[i, j]) * mid - beside)
            d2 = (FACTOR2 * FACTOR1) * mid + (2.0 * FACTOR2 / HALF) * r
            emit(i, j, u[i, j] + d0[i, j] + mid + d2)
        row_done(i)
        return carry

    lax.fori_loop(low + 1, low + 5 + rows, first, 0)
    lax.fori_loop(low + 2, low + 4 + rows, second, 0)
    lax.fori_loop(low + 3, low + 3 + rows, third, 0)


def prolong_cell(lines, index, blocks, guess, a, b):
    pair = jnp.concatenate([lines[index(a, b, k)] for k in range(2)], axis=1)
    both = jnp.concatenate([blocks[a, b, k] for k in range(2)], axis=1)
    return guess[a, b] + lax.dot_general(pair, both, (((1,), (1,)), ((), ())), preferred_element_type=F32)


VMEM = pl.BlockSpec(memory_space=pltpu.VMEM)
HBM = pl.BlockSpec(memory_space=pltpu.HBM)


def fetch(sems, *pairs):
    copies = [pltpu.make_async_copy(a, b, sems.at[n]) for n, (a, b) in enumerate(pairs)]
    for copy in copies:
        copy.start()
    return copies


def fetched(*arrays):
    return [pltpu.VMEM(x.shape, x.dtype) for x in arrays] + [pltpu.SemaphoreType.DMA((len(arrays) + 1,))]


def smem_last(*arrays):
    *first, sems = fetched(*arrays)
    return [*first[:-1], pltpu.SMEM(arrays[-1].shape, arrays[-1].dtype), sems]


def call(kernel, inputs, outs, scratch, flops, vmem=16, hbm=(), out=None):
    nbytes = sum(x.size * x.dtype.itemsize for x in inputs)
    specs = [HBM if n in hbm else VMEM for n in range(len(inputs))]
    inputs = [pltpu.with_memory_space_constraint(x, pltpu.HBM) if n in hbm else x for n, x in enumerate(inputs)]
    return pl.pallas_call(
        kernel,
        out_shape=outs,
        in_specs=specs,
        out_specs=tuple(out or VMEM for _ in outs),
        scratch_shapes=scratch,
        compiler_params=pltpu.CompilerParams(vmem_limit_bytes=vmem << 20),
        cost_estimate=pl.CostEstimate(flops=flops, bytes_accessed=nbytes, transcendentals=0),
    )(*inputs)


def cells(rows, cols, dtype=F32):
    return pltpu.VMEM((rows, cols, R, L), dtype)


def shifts(rows, cols):
    return pltpu.VMEM((rows, cols, 1, L), F32)


def pack_kernel(source_fourth, guess_fourth, shift_fourth, shift_third, source_third, out, s4, s3, sems):
    pairs = [(shift_fourth, s4), (shift_third, s3), (source_fourth.at[0, 0], out.at[0:16]), (guess_fourth.at[0, 0], out.at[16:32])]
    for i in range(2):
        for j in range(2):
            at = 40 + (i * 2 + j) * R
            pairs.append((source_third.at[i, j], out.at[at : at + R]))
    copies = fetch(sems, *pairs)
    copies[0].wait()
    copies[1].wait()
    out[32:33, :] = s4[0]
    for i in range(2):
        out[33 + 2 * i : 35 + 2 * i, :] = s3[i]
    out[37:40, :] = jnp.zeros((3, L), F32)
    for copy in copies[2:]:
        copy.wait()


THIRD = 1232


def ahead_kernel(
    source_first_h, shift_first_h, source_second_h, shift_second_h, blocks_third, guess_third_h, links_third,
    third, own, even, odd, row_on, row_off,
    source_first, shift_first, source_second, shift_second, guess_third, links, sems,
):
    pairs = [
        (links_third, links), (guess_third_h, guess_third), (source_second_h, source_second), (shift_second_h, shift_second),
        (shift_first_h, shift_first), (source_first_h, source_first),
    ]
    for c in range(8):
        pairs.append((blocks_third.at[c // 4, c // 2 % 2, c % 2], third.at[c * L : (c + 1) * L]))
    copies = fetch(sems, *pairs)
    for copy in copies[:6]:
        copy.wait()
    for i in range(2):
        for j in range(2):
            rest = guess_third[i, j]
            for n in range(3):
                term = rest.astype(BF16)
                at = 1024 + n * 64 + (i * 2 + j) * R
                third[at : at + R, :] = term
                rest = rest - term.astype(F32)
    names = lax.broadcasted_iota(jnp.int32, (16, L), 0)
    rows = jnp.zeros((16, L), jnp.int32)
    for c in range(8):
        rows = jnp.where(names == c, links[c // 4, c // 2 % 2, c % 2], rows)
    third[1216:1232, :] = rows.astype(F32).astype(BF16)

    side, core = lax.rem(lax.axis_index("gy"), 2), lax.rem(lax.axis_index("gz"), 2)
    for i in range(4):
        for j in range(4):
            at = (i * 4 + j) * R
            own[at : at + R, :] = source_second[i, j]
        own[256 + i * 4 : 260 + i * 4, :] = shift_second[i]
    for ref, first in ((even, 6 - 6 * side), (odd, 6 * side)):
        ref[0:272, :] = own[...]
        for i in range(8):
            for j in range(2):
                at = 272 + (i * 2 + j) * R
                ref[at : at + R, :] = source_first[i, first + j]
            ref[528 + i * 2 : 530 + i * 2, :] = jnp.where(first == 0, shift_first[i, 0:2, :], shift_first[i, 6:8, :])
    for ref, first in ((row_on, 6 - 6 * core), (row_off, 6 * core)):
        for i in range(2):
            for j in range(8):
                at = (i * 8 + j) * R
                ref[at : at + R, :] = source_first[first + i, j]
            ref[256 + i * 8 : 264 + i * 8, :] = shift_first[first + i]
    for copy in copies[6:]:
        copy.wait()


def relay_kernel(near, far, out):
    out[0] = near[...]
    out[1] = far[...]


def fourth_kernel(pair, a, a3, both, third0, third1, third2, third3, out, start, u, f, s, res, d0, d1, lines):
    gz, gy = lax.axis_index("gz"), lax.axis_index("gy")
    core = lax.rem(gz, 2)

    def place(ref, chip, first_bit):
        for slot in range(2):
            bit = first_bit if slot == 0 else 1 - first_bit
            row = chip * 2 + bit
            for k in range(4):
                col = lax.bitwise_xor(gy, k)
                f[row, col] = ref[slot, k, 0:16, :]
                u[row, col] = ref[slot, k, 16:32, :]
                s[row, col] = ref[slot, k, 32:33, :]

    place(pair, 2, core)
    place(a, 1 + 2 * core, 1 - core)
    place(both.at[0], 3 - 2 * core, core)
    place(a3, 4 * core, 1 - core)
    place(both.at[1], 4 - 4 * core, core)

    def emit(i, j, value):
        lines[i - 3 - core, j] = value.astype(BF16).astype(F32)
        res[i, j] = value

    smooth(u, f, s, res, d0, d1, emit, core, 3, 4, True)
    out[0, 0] = res[4 + core, gy]

    for n, ref in enumerate((third0, third1, third2, third3)):
        col = lax.bitwise_xor(gy, n) * 2
        for c in range(4):
            i, j = c // 2, c % 2
            at = 1024 + c * R
            total = (ref[at : at + R, :].astype(F32) + ref[at + 64 : at + 64 + R, :].astype(F32)) + ref[at + 128 : at + 128 + R, :].astype(F32)
            names = ref[1216:1232, :].astype(F32)
            for k in range(2):
                name = names[c * 2 + k : c * 2 + k + 1, :]
                line = jnp.zeros((R, L), F32)
                for row in range(3):
                    base = (lax.rem(gz + row - 1 + NZ, NZ) * 4).astype(F32)
                    for x in range(4):
                        line = jnp.where(jnp.broadcast_to(name == base + x, (R, L)), lines[row, x], line)
                at = (c * 2 + k) * L
                total = total + lax.dot_general(
                    line.astype(BF16), ref[at : at + L, :], (((1,), (1,)), ((), ())), preferred_element_type=F32
                )
            start[pl.ds(pl.multiple_of((i * 8 + col + j) * R, R), R), :] = total


def third_kernel(pair, a, b, fpair, fa, fb, spair, sa, sb, links_h, blocks, guess_h, out, start, u, f, s, res, d0, d1, lines, guess, links, sems):
    copies = fetch(sems, (guess_h, guess), (links_h, links))
    gz, gy = lax.axis_index("gz"), lax.axis_index("gy")
    core = lax.rem(gz, 2)

    def place(ref, fref, sref, chip, first_bit):
        for slot in range(2):
            bit = first_bit if slot == 0 else 1 - first_bit
            for k in range(4):
                col = lax.bitwise_xor(gy, k) * 2
                for i in range(2):
                    row = chip * 4 + bit * 2 + i
                    for j in range(2):
                        at = (i * 2 + j) * R
                        f[row, col + j] = fref[slot, k, at : at + R, :]
                        s[row, col + j] = sref[slot, k, 33 + i * 2 + j : 34 + i * 2 + j, :]
            for i in range(2):
                for j in range(8):
                    at = (i * 8 + j) * R
                    u[chip * 4 + bit * 2 + i, j] = ref[slot, at : at + R, :]

    place(pair, fpair, spair, 1, core)
    place(a, fa, sa, 2 * core, 1 - core)
    place(b, fb, sb.at[0], 2 - 2 * core, core)

    def emit(i, j, value):
        lines[i - 3 - 2 * core, j] = value.astype(BF16)
        res[i, j] = value

    smooth(u, f, s, res, d0, d1, emit, 2 * core, 4, 8, True)
    for i in range(2):
        for j in range(2):
            out[i, j] = res[4 + 2 * core + i, 2 * gy + j]

    for copy in copies:
        copy.wait()

    def index(i, j, k):
        q = links[i, k, j]
        return lax.rem(q // 8 - 2 * gz + 1 + 2 * NZ, 2 * NZ), lax.rem(q, 8)

    for i in range(4):
        for j in range(4):
            start[i, j] = prolong_cell(lines, index, blocks, guess, i, j)


ALONG_Y, ALONG_Z = 544, 1224


def along_z_kernel(own, even, odd, row_on, row_off, on, off):
    core = lax.rem(lax.axis_index("gz"), 2)
    for ref, rows, first in ((on, row_on, 6 - 6 * core), (off, row_off, 6 * core)):
        ref[0:272, :] = own[...]
        ref[272:544, :] = even[0:272, :]
        ref[544:816, :] = odd[0:272, :]
        for i in range(2):
            row = first + i
            at = 816 + i * 12 * R
            ref[at : at + 8 * R, :] = rows[i * 8 * R : (i + 1) * 8 * R, :]
            ref[1200 + i * 12 : 1208 + i * 12, :] = rows[256 + i * 8 : 264 + i * 8, :]
            for n, side_ref in enumerate((even, odd)):
                at = 816 + (i * 12 + 8 + 2 * n) * R
                ref[at : at + 2 * R, :] = side_ref[pl.ds(pl.multiple_of(272 + row * 2 * R, 8), 2 * R), :]
                low = side_ref[528 + 2 * i : 530 + 2 * i, :]
                high = side_ref[540 + 2 * i : 542 + 2 * i, :]
                ref[1208 + i * 12 + 2 * n : 1210 + i * 12 + 2 * n, :] = jnp.where(first == 0, low, high)


SIDE4 = tuple((r, n) for r in range(4) for n in range(4 - r))
BLOCK = (16 + 2 * len(SIDE4)) * R


def at_cell(ref, cell):
    return ref[pl.ds(pl.multiple_of(cell * R, R), R), :]


def block_kernel(own, even, odd, on, off):
    core, side = lax.rem(lax.axis_index("gz"), 2), lax.rem(lax.axis_index("gy"), 2)
    for ref, right in ((on, 1 - core), (off, core)):
        for r in range(4):
            row = r + right * (3 - 2 * r)
            for j in range(4):
                at = (r * 4 + j) * R
                ref[at : at + R, :] = at_cell(own, row * 4 + j)
        for m, (r, n) in enumerate(SIDE4):
            row = r + right * (3 - 2 * r)
            for k, (beside, left) in enumerate(((even, side), (odd, 1 - side))):
                at = (16 + k * len(SIDE4) + m) * R
                ref[at : at + R, :] = at_cell(beside, row * 4 + n + left * (3 - 2 * n))


def second_kernel(own, own_even, own_odd, on, off, fown, feven, fodd, fon, foff, links_h, blocks, guess, out, start, even, odd, u, f, s, res, d0, d1, lines, links, sems):
    copies = fetch(sems, (links_h, links))
    gz, gy = lax.axis_index("gz"), lax.axis_index("gy")
    core, side = lax.rem(gz, 2), lax.rem(gy, 2)
    starts = (4, 8 - 8 * side, 8 * side)

    def place(frefs, row0):
        for k in range(3):
            fref, fbase = frefs[k]
            for i in range(4):
                for j in range(4):
                    c = i * 4 + j
                    row, col = row0 + i, starts[k] + j
                    f[row, col] = fref[fbase + c * R : fbase + (c + 1) * R, :]
                    s[row, col] = fref[fbase + 256 + c : fbase + 257 + c, :]

    place(((fown, 0), (feven, 0), (fodd, 0)), 4)
    for fref, row0 in ((fon, 8 - 8 * core), (foff, 8 * core)):
        place([(fref, 272 * k) for k in range(3)], row0)
    for i in range(4):
        for j in range(4):
            at = (i * 4 + j) * R
            for k, ref in enumerate((own, own_even, own_odd)):
                u[4 + i, starts[k] + j] = ref[at : at + R, :]
    for ref, left in ((on, core), (off, 1 - core)):
        for r in range(4):
            row = 8 + r - left * (5 + 2 * r)
            for j in range(4):
                at = (r * 4 + j) * R
                u[row, 4 + j] = ref[at : at + R, :]
        for m, (r, n) in enumerate(SIDE4):
            row = 8 + r - left * (5 + 2 * r)
            for k, across in enumerate((side, 1 - side)):
                at = (16 + k * len(SIDE4) + m) * R
                u[row, 8 + n - across * (5 + 2 * n)] = ref[at : at + R, :]

    def emit(i, j, value):
        lines[i - 3, j - 3] = value.astype(BF16)
        res[i, j] = value

    smooth(u, f, s, res, d0, d1, emit, 0, 6, 12, False)
    for i in range(4):
        for j in range(4):
            out[i, j] = res[4 + i, 4 + j]

    for copy in copies:
        copy.wait()

    def index(i, j, k):
        q = links[i, k, j]
        row = lax.rem(q // 16 - 4 * gz + 1 + 4 * NZ, 4 * NZ)
        return row, lax.rem(lax.rem(q, 16) - 4 * gy + 1 + 4 * NY, 4 * NY)

    def row_of_cells(i, carry):
        for j in range(8):
            start[i, j] = prolong_cell(lines, index, blocks, guess, i, j)
        return carry

    lax.fori_loop(0, 8, row_of_cells, 0)
    for i in range(8):
        for j in range(3):
            at = (i * 3 + j) * R
            even[at : at + R, :] = start[i, 5 - 5 * side + j]
            odd[at : at + R, :] = start[i, 5 * side + j]


SIDE3 = ((0, 0), (0, 1), (1, 0))
ROWS = (24 + 2 * len(SIDE3)) * R


def rows_kernel(start, even, odd, on, off):
    core, side = lax.rem(lax.axis_index("gz"), 2), lax.rem(lax.axis_index("gy"), 2)
    for ref, right in ((on, 1 - core), (off, core)):
        for r in range(3):
            row = r + right * (7 - 2 * r)
            for j in range(8):
                at = (r * 8 + j) * R
                ref[at : at + R, :] = start[row, j]
        for m, (r, n) in enumerate(SIDE3):
            row = r + right * (7 - 2 * r)
            for k, (beside, left) in enumerate(((even, side), (odd, 1 - side))):
                at = (24 + k * len(SIDE3) + m) * R
                ref[at : at + R, :] = at_cell(beside, row * 3 + n + left * (2 - 2 * n))


def first_kernel(own, even, odd, on, off, fown, sown, feven, fodd, fon, foff, out, u, f, s, res, d0, d1, done, sems):
    gz, gy = lax.axis_index("gz"), lax.axis_index("gy")
    core, side = lax.rem(gz, 2), lax.rem(gy, 2)
    even_u, odd_u = 11 - 11 * side, 11 * side
    even_f, odd_f = 11 - 10 * side, 1 + 10 * side

    for i in range(8):
        for j in range(8):
            u[3 + i, 3 + j] = own[i, j]
            f[3 + i, 3 + j] = fown[i, j]
            s[3 + i, 3 + j] = sown[i, j : j + 1, :]
        for j in range(3):
            at = (i * 3 + j) * R
            u[3 + i, even_u + j] = even[at : at + R, :]
            u[3 + i, odd_u + j] = odd[at : at + R, :]
        for j in range(2):
            c = i * 2 + j
            at = 272 + c * R
            f[3 + i, even_f + j] = feven[at : at + R, :]
            f[3 + i, odd_f + j] = fodd[at : at + R, :]
            s[3 + i, even_f + j] = feven[528 + c : 529 + c, :]
            s[3 + i, odd_f + j] = fodd[528 + c : 529 + c, :]

    def place(ref, fref, left, row_f):
        for r in range(3):
            for j in range(8):
                at = (r * 8 + j) * R
                u[11 + r - left * (9 + 2 * r), 3 + j] = ref[at : at + R, :]
        for m, (r, n) in enumerate(SIDE3):
            for k, across in enumerate((side, 1 - side)):
                at = (24 + k * len(SIDE3) + m) * R
                u[11 + r - left * (9 + 2 * r), 11 + n - across * (9 + 2 * n)] = ref[at : at + R, :]
        for i in range(2):
            for j in range(12):
                col = 3 + j if j < 8 else even_f + j - 8 if j < 10 else odd_f + j - 10
                c = i * 12 + j
                at = 816 + c * R
                f[row_f + i, col] = fref[at : at + R, :]
                s[row_f + i, col] = fref[1200 + c : 1201 + c, :]

    place(on, fon, core, 11 - 10 * core)
    place(off, foff, 1 - core, 1 + 10 * core)

    def emit(i, j, value):
        done[i - 3, j - 3] = value

    def leave(i):
        return pltpu.make_async_copy(done.at[i], out.at[i], sems.at[i])

    smooth(u, f, s, res, d0, d1, emit, 0, 8, 14, False, lambda i: leave(i - 3).start())
    for i in range(8):
        leave(i).wait()


def onchip(*shape):
    return pltpu.VMEM(shape, F32)


def sds(*shape, dtype=F32):
    return jax.ShapeDtypeStruct(shape, dtype)


def flat(x):
    return x.reshape(-1, L)


def shards(
    source_first, source_second, source_third, source_fourth,
    guess_first, guess_second, guess_third, guess_fourth,
    shift_first, shift_second, shift_third, shift_fourth,
    blocks_first, blocks_second, blocks_third,
    links_first, links_second, links_third,
):
    links_first, links_second = links_first.transpose(0, 2, 1), links_second.transpose(0, 2, 1)

    (pack,) = call(
        pack_kernel,
        (source_fourth, guess_fourth, shift_fourth, shift_third, source_third),
        (sds(104, L),),
        [pltpu.VMEM((1, 1, L), F32), pltpu.VMEM((2, 2, L), F32), pltpu.SemaphoreType.DMA((8,))],
        1000, 2, range(5),
    )
    y1 = y_by(pack, 1)
    y2 = y_by(pack, 2)
    y3 = y_by(pack, 3)
    line = jnp.stack([pack, y1, y2, y3])
    line_on = z_on(line)
    pair = jnp.stack([line[:, :40], line_on[:, :40]])
    pair_f = jnp.stack([line[:, 40:], line_on[:, 40:]])
    near = z_off(pair)
    far = z_off3(pair)
    (both,) = call(relay_kernel, (near, far), (sds(2, 2, 4, 40, L),), [], 1000, 2)
    both = z_on(both)
    near_f = z_off(pair_f)
    near_fb = z_on(near_f)

    third, mine, ahead_even, ahead_odd, row_on, row_off = call(
        ahead_kernel,
        (source_first, shift_first, source_second, shift_second, blocks_third, guess_third, links_third),
        (sds(THIRD, L, dtype=BF16), sds(272, L), sds(ALONG_Y, L), sds(ALONG_Y, L), sds(272, L), sds(272, L)),
        [pltpu.VMEM(x.shape, x.dtype) for x in (source_first, shift_first, source_second, shift_second, guess_third)]
        + [pltpu.SMEM(links_third.shape, jnp.int32), pltpu.SemaphoreType.DMA((16,))],
        1000, 6, range(7),
    )
    third1 = y_by(third, 1)
    third2 = y_by(third, 2)
    third3 = y_by(third, 3)
    ahead_even = y_even(ahead_even)
    ahead_odd = y_odd(ahead_odd)
    ahead_on, ahead_off = call(
        along_z_kernel,
        (mine, ahead_even, ahead_odd, row_on, row_off),
        (sds(ALONG_Z, L), sds(ALONG_Z, L)),
        [], 10000, 6,
    )
    ahead_on = z_on(ahead_on)
    ahead_off = z_off(ahead_off)

    def smoothing_scratch(rows, cols):
        return [cells(rows, cols), cells(rows, cols), shifts(rows, cols)] + [cells(rows, cols)] * 3

    out_fourth, start_third = call(
        fourth_kernel,
        (pair, near, far, both, third, third1, third2, third3),
        (onchip(1, 1, R, L), sds(256, L)),
        smoothing_scratch(10, 4) + [cells(3, 4)],
        4_000_000, 6,
    )

    start_on = z_on(start_third)
    pair3 = jnp.stack([start_third, start_on])
    near3 = z_off(pair3)
    near3_b = z_on(near3)
    out_third, start_second = call(
        third_kernel,
        (pair3, near3, near3_b, pair_f, near_f, near_fb, pair, near, both, links_second, blocks_second, guess_second),
        (onchip(2, 2, R, L), sds(4, 4, R, L)),
        smoothing_scratch(12, 8) + [cells(4, 8, BF16)] + smem_last(guess_second, links_second),
        8_000_000, 12, (9, 11),
    )

    own = flat(start_second)
    own_even, own_odd = y_even(own), y_odd(own)
    block_on, block_off = call(block_kernel, (own, own_even, own_odd), (sds(BLOCK, L), sds(BLOCK, L)), [], 10000, 4)
    out_second, start_first, strip_even, strip_odd = call(
        second_kernel,
        (own, own_even, own_odd, z_on(block_on), z_off(block_off), mine, ahead_even, ahead_odd, ahead_on, ahead_off, links_first, blocks_first, guess_first),
        (onchip(4, 4, R, L), sds(8, 8, R, L), sds(24 * R, L), sds(24 * R, L)),
        smoothing_scratch(12, 12) + [cells(6, 6, BF16)] + smem_last(links_first),
        16_000_000, 20, (10,),
    )

    u_even, u_odd = y_even(strip_even), y_odd(strip_odd)
    u_on, u_off = call(rows_kernel, (start_first, u_even, u_odd), (sds(ROWS, L), sds(ROWS, L)), [], 10000, 4)
    (out_first,) = call(
        first_kernel,
        (start_first, u_even, u_odd, z_on(u_on), z_off(u_off), source_first, shift_first, ahead_even, ahead_odd, ahead_on, ahead_off),
        (sds(8, 8, R, L),),
        smoothing_scratch(14, 14) + [cells(8, 8), pltpu.SemaphoreType.DMA((8,))],
        16_000_000, 20, (), HBM,
    )
    return out_first, out_second, out_third, out_fourth


def solution(mesh):
    field = P("gz", "gy", None, None)
    line = P("gz", "gy", None)
    block = P("gz", "gy", None, None, None)

    return jax.shard_map(
        shards,
        mesh=mesh,
        in_specs=(field,) * 8 + (line,) * 4 + (block,) * 3 + (line,) * 3,
        out_specs=(field,) * 4,
        check_vma=False,
    )
```

```python
import jax
import jax.numpy as jnp
from jax import lax
from jax.experimental import pallas as pl
from jax.experimental.pallas import tpu as pltpu
from jax.sharding import PartitionSpec as P


UPPER = 14.0
LOWER = UPPER / 8.0
CENTRE = (UPPER + LOWER) / 2.0
HALF = (UPPER - LOWER) / 2.0
RATIO = CENTRE / HALF
FACTOR0 = 1.0 / RATIO
FACTOR1 = 1.0 / (2.0 * RATIO - FACTOR0)
FACTOR2 = 1.0 / (2.0 * RATIO - FACTOR1)

F32 = jnp.float32
BF16 = jnp.bfloat16
R = 16
L = 128

NZ, NY = 64, 4


def swap(x, axis, partner):
    return lax.ppermute(x, axis, [(i, partner(i)) for i in range(lax.axis_size(axis))])


def z_on(x):
    return swap(x, "gz", lambda i: i ^ 1)


def z_off(x):
    return swap(x, "gz", lambda i: (((i + 1) ^ 1) - 1) % NZ)


def z_off3(x):
    return swap(x, "gz", lambda i: (i - 3 if i % 2 == 0 else i + 3) % NZ)


def y_by(x, k):
    return swap(x, "gy", lambda j: j ^ k)


def y_even(x):
    return y_by(x, 1)


def y_odd(x):
    return y_by(x, 3)


def neighbours(v, i, j, width, wrap):
    jl = (j - 1) % width if wrap else j - 1
    jr = (j + 1) % width if wrap else j + 1
    mid = v[i, j]
    beside = v[i - 1, j] + v[i + 1, j] + v[i, jl] + v[i, jr]
    beside = beside + pltpu.roll(mid, 1, 1) + pltpu.roll(mid, L - 1, 1)
    return mid, beside


def smooth(u, f, s, res, d0, d1, emit, low, rows, width, wrap, row_done=lambda i: None):
    def columns(k):
        return range(width) if wrap else range(k, width - k)

    def first(i, carry):
        for j in columns(1):
            mid, beside = neighbours(u, i, j, width, wrap)
            r = f[i, j] - ((6.0 + s[i, j]) * mid - beside)
            res[i, j] = r
            d0[i, j] = r * (1.0 / CENTRE)
        return carry

    def second(i, carry):
        for j in columns(2):
            mid, beside = neighbours(d0, i, j, width, wrap)
            r = res[i, j] - ((6.0 + s[i, j]) * mid - beside)
            res[i, j] = r
            d1[i, j] = (FACTOR1 * FACTOR0) * mid + (2.0 * FACTOR1 / HALF) * r
        return carry

    def third(i, carry):
        for j in columns(3):
            mid, beside = neighbours(d1, i, j, width, wrap)
            r = res[i, j] - ((6.0 + s[i, j]) * mid - beside)
            d2 = (FACTOR2 * FACTOR1) * mid + (2.0 * FACTOR2 / HALF) * r
            emit(i, j, u[i, j] + d0[i, j] + mid + d2)
        row_done(i)
        return carry

    lax.fori_loop(low + 1, low + 5 + rows, first, 0)
    lax.fori_loop(low + 2, low + 4 + rows, second, 0)
    lax.fori_loop(low + 3, low + 3 + rows, third, 0)


def prolong_cell(lines, index, blocks, guess, a, b):
    pair = jnp.concatenate([lines[index(a, b, k)] for k in range(2)], axis=1)
    both = jnp.concatenate([blocks[a, b, k] for k in range(2)], axis=1)
    return guess[a, b] + lax.dot_general(pair, both, (((1,), (1,)), ((), ())), preferred_element_type=F32)


VMEM = pl.BlockSpec(memory_space=pltpu.VMEM)
HBM = pl.BlockSpec(memory_space=pltpu.HBM)


def fetch(sems, *pairs):
    copies = [pltpu.make_async_copy(a, b, sems.at[n]) for n, (a, b) in enumerate(pairs)]
    for copy in copies:
        copy.start()
    return copies


def fetched(*arrays):
    return [pltpu.VMEM(x.shape, x.dtype) for x in arrays] + [pltpu.SemaphoreType.DMA((len(arrays) + 1,))]


def smem_last(*arrays):
    *first, sems = fetched(*arrays)
    return [*first[:-1], pltpu.SMEM(arrays[-1].shape, arrays[-1].dtype), sems]


def call(kernel, inputs, outs, scratch, flops, vmem=16, hbm=(), out=None):
    nbytes = sum(x.size * x.dtype.itemsize for x in inputs)
    specs = [HBM if n in hbm else VMEM for n in range(len(inputs))]
    inputs = [pltpu.with_memory_space_constraint(x, pltpu.HBM) if n in hbm else x for n, x in enumerate(inputs)]
    return pl.pallas_call(
        kernel,
        out_shape=outs,
        in_specs=specs,
        out_specs=tuple(out or VMEM for _ in outs),
        scratch_shapes=scratch,
        compiler_params=pltpu.CompilerParams(vmem_limit_bytes=vmem << 20),
        cost_estimate=pl.CostEstimate(flops=flops, bytes_accessed=nbytes, transcendentals=0),
    )(*inputs)


def cells(rows, cols, dtype=F32):
    return pltpu.VMEM((rows, cols, R, L), dtype)


def shifts(rows, cols):
    return pltpu.VMEM((rows, cols, 1, L), F32)


def pack_kernel(source_fourth, guess_fourth, shift_fourth, shift_third, source_third, out, s4, s3, sems):
    pairs = [(shift_fourth, s4), (shift_third, s3), (source_fourth.at[0, 0], out.at[0:16]), (guess_fourth.at[0, 0], out.at[16:32])]
    for i in range(2):
        for j in range(2):
            at = 40 + (i * 2 + j) * R
            pairs.append((source_third.at[i, j], out.at[at : at + R]))
    copies = fetch(sems, *pairs)
    copies[0].wait()
    copies[1].wait()
    out[32:33, :] = s4[0]
    for i in range(2):
        out[33 + 2 * i : 35 + 2 * i, :] = s3[i]
    out[37:40, :] = jnp.zeros((3, L), F32)
    for copy in copies[2:]:
        copy.wait()


THIRD = 1232


def ahead_kernel(
    source_first_h, shift_first_h, source_second_h, shift_second_h, blocks_third, guess_third_h, links_third,
    third, own, even, odd, row_low, row_high,
    source_first, shift_first, source_second, shift_second, guess_third, links, sems,
):
    pairs = [
        (links_third, links), (guess_third_h, guess_third), (source_second_h, source_second), (shift_second_h, shift_second),
        (shift_first_h, shift_first), (source_first_h, source_first),
    ]
    for c in range(8):
        pairs.append((blocks_third.at[c // 4, c // 2 % 2, c % 2], third.at[c * L : (c + 1) * L]))
    copies = fetch(sems, *pairs)
    for copy in copies[:6]:
        copy.wait()
    for i in range(2):
        for j in range(2):
            rest = guess_third[i, j]
            for n in range(3):
                term = rest.astype(BF16)
                at = 1024 + n * 64 + (i * 2 + j) * R
                third[at : at + R, :] = term
                rest = rest - term.astype(F32)
    names = lax.broadcasted_iota(jnp.int32, (16, L), 0)
    rows = jnp.zeros((16, L), jnp.int32)
    for c in range(8):
        rows = jnp.where(names == c, links[c // 4, c // 2 % 2, c % 2], rows)
    third[1216:1232, :] = rows.astype(F32).astype(BF16)

    side = lax.rem(lax.axis_index("gy"), 2)
    for i in range(4):
        for j in range(4):
            at = (i * 4 + j) * R
            own[at : at + R, :] = source_second[i, j]
        own[256 + i * 4 : 260 + i * 4, :] = shift_second[i]
    for ref, first in ((even, 6 - 6 * side), (odd, 6 * side)):
        ref[0:272, :] = own[...]
        for i in range(8):
            for j in range(2):
                at = 272 + (i * 2 + j) * R
                ref[at : at + R, :] = source_first[i, first + j]
            ref[528 + i * 2 : 530 + i * 2, :] = jnp.where(first == 0, shift_first[i, 0:2, :], shift_first[i, 6:8, :])
    for ref, first in ((row_low, 0), (row_high, 6)):
        for i in range(2):
            for j in range(8):
                at = (i * 8 + j) * R
                ref[at : at + R, :] = source_first[first + i, j]
            ref[256 + i * 8 : 264 + i * 8, :] = shift_first[first + i]
    for copy in copies[6:]:
        copy.wait()


def pair_kernel(line, line_on, pair, short):
    for slot, ref in enumerate((line, line_on)):
        pair[slot] = ref[...]
        short[slot] = ref[:, 0:40, :]


def relay_kernel(near, far, out):
    out[:, :, 0:104, :] = near[...]
    out[:, :, 104:144, :] = far[...]


def pick_kernel(low, high, on, off):
    core = lax.rem(lax.axis_index("gz"), 2)
    on[...] = jnp.where(core == 0, high[...], low[...])
    off[...] = jnp.where(core == 0, low[...], high[...])


def fourth_kernel(pair, a, a3, both, third0, third1, third2, third3, out, start, u, f, s, res, d0, d1, lines):
    gz, gy = lax.axis_index("gz"), lax.axis_index("gy")
    core = lax.rem(gz, 2)

    def place(ref, chip, first_bit, at=0):
        for slot in range(2):
            bit = first_bit if slot == 0 else 1 - first_bit
            row = chip * 2 + bit
            for k in range(4):
                col = lax.bitwise_xor(gy, k)
                f[row, col] = ref[slot, k, at : at + 16, :]
                u[row, col] = ref[slot, k, at + 16 : at + 32, :]
                s[row, col] = ref[slot, k, at + 32 : at + 33, :]

    place(pair, 2, core)
    place(a, 1 + 2 * core, 1 - core)
    place(both, 3 - 2 * core, core)
    place(a3, 4 * core, 1 - core)
    place(both, 4 - 4 * core, core, 104)

    def emit(i, j, value):
        lines[i - 3 - core, j] = value.astype(BF16).astype(F32)
        res[i, j] = value

    smooth(u, f, s, res, d0, d1, emit, core, 3, 4, True)
    out[0, 0] = res[4 + core, gy]

    for n, ref in enumerate((third0, third1, third2, third3)):
        col = lax.bitwise_xor(gy, n) * 2
        for c in range(4):
            i, j = c // 2, c % 2
            at = 1024 + c * R
            total = (ref[at : at + R, :].astype(F32) + ref[at + 64 : at + 64 + R, :].astype(F32)) + ref[at + 128 : at + 128 + R, :].astype(F32)
            names = ref[1216:1232, :].astype(F32)
            for k in range(2):
                name = names[c * 2 + k : c * 2 + k + 1, :]
                line = jnp.zeros((R, L), F32)
                for row in range(3):
                    base = (lax.rem(gz + row - 1 + NZ, NZ) * 4).astype(F32)
                    for x in range(4):
                        line = jnp.where(jnp.broadcast_to(name == base + x, (R, L)), lines[row, x], line)
                at = (c * 2 + k) * L
                total = total + lax.dot_general(
                    line.astype(BF16), ref[at : at + L, :], (((1,), (1,)), ((), ())), preferred_element_type=F32
                )
            start[pl.ds(pl.multiple_of((i * 8 + col + j) * R, R), R), :] = total


def third_kernel(pair, a, b, fpair, fa, fb, links_h, blocks, guess_h, out, start, u, f, s, res, d0, d1, lines, guess, links, sems):
    copies = fetch(sems, (guess_h, guess), (links_h, links))
    gz, gy = lax.axis_index("gz"), lax.axis_index("gy")
    core = lax.rem(gz, 2)

    def place(ref, fref, chip, first_bit):
        for slot in range(2):
            bit = first_bit if slot == 0 else 1 - first_bit
            for k in range(4):
                col = lax.bitwise_xor(gy, k) * 2
                for i in range(2):
                    row = chip * 4 + bit * 2 + i
                    for j in range(2):
                        at = (i * 2 + j) * R
                        f[row, col + j] = fref[slot, k, 40 + at : 40 + at + R, :]
                        s[row, col + j] = fref[slot, k, 33 + i * 2 + j : 34 + i * 2 + j, :]
            for i in range(2):
                for j in range(8):
                    at = (i * 8 + j) * R
                    u[chip * 4 + bit * 2 + i, j] = ref[slot, at : at + R, :]

    place(pair, fpair, 1, core)
    place(a, fa, 2 * core, 1 - core)
    place(b, fb, 2 - 2 * core, core)

    def emit(i, j, value):
        lines[i - 3 - 2 * core, j] = value.astype(BF16)
        res[i, j] = value

    smooth(u, f, s, res, d0, d1, emit, 2 * core, 4, 8, True)
    for i in range(2):
        for j in range(2):
            out[i, j] = res[4 + 2 * core + i, 2 * gy + j]

    for copy in copies:
        copy.wait()

    def index(i, j, k):
        q = links[i, k, j]
        return lax.rem(q // 8 - 2 * gz + 1 + 2 * NZ, 2 * NZ), lax.rem(q, 8)

    for i in range(4):
        for j in range(4):
            start[i, j] = prolong_cell(lines, index, blocks, guess, i, j)


ALONG_Y, ALONG_Z = 544, 1224


def along_z_kernel(own, even, odd, row_on, row_off, on, off):
    core = lax.rem(lax.axis_index("gz"), 2)
    for ref, rows, first in ((on, row_on, 6 - 6 * core), (off, row_off, 6 * core)):
        ref[0:272, :] = own[...]
        ref[272:544, :] = even[0:272, :]
        ref[544:816, :] = odd[0:272, :]
        for i in range(2):
            row = first + i
            at = 816 + i * 12 * R
            ref[at : at + 8 * R, :] = rows[i * 8 * R : (i + 1) * 8 * R, :]
            ref[1200 + i * 12 : 1208 + i * 12, :] = rows[256 + i * 8 : 264 + i * 8, :]
            for n, side_ref in enumerate((even, odd)):
                at = 816 + (i * 12 + 8 + 2 * n) * R
                ref[at : at + 2 * R, :] = side_ref[pl.ds(pl.multiple_of(272 + row * 2 * R, 8), 2 * R), :]
                low = side_ref[528 + 2 * i : 530 + 2 * i, :]
                high = side_ref[540 + 2 * i : 542 + 2 * i, :]
                ref[1208 + i * 12 + 2 * n : 1210 + i * 12 + 2 * n, :] = jnp.where(first == 0, low, high)


SIDE4 = tuple((r, n) for r in range(4) for n in range(4 - r))
BLOCK = (16 + 2 * len(SIDE4)) * R


def at_cell(ref, cell):
    return ref[pl.ds(pl.multiple_of(cell * R, R), R), :]


def block_kernel(own, even, odd, on, off):
    core, side = lax.rem(lax.axis_index("gz"), 2), lax.rem(lax.axis_index("gy"), 2)
    for ref, right in ((on, 1 - core), (off, core)):
        for r in range(4):
            row = r + right * (3 - 2 * r)
            for j in range(4):
                at = (r * 4 + j) * R
                ref[at : at + R, :] = at_cell(own, row * 4 + j)
        for m, (r, n) in enumerate(SIDE4):
            row = r + right * (3 - 2 * r)
            for k, (beside, left) in enumerate(((even, side), (odd, 1 - side))):
                at = (16 + k * len(SIDE4) + m) * R
                ref[at : at + R, :] = at_cell(beside, row * 4 + n + left * (3 - 2 * n))


def second_kernel(own, own_even, own_odd, on, off, fown, feven, fodd, fon, foff, links_h, blocks, guess, out, start, even, odd, u, f, s, res, d0, d1, lines, links, sems):
    copies = fetch(sems, (links_h, links))
    gz, gy = lax.axis_index("gz"), lax.axis_index("gy")
    core, side = lax.rem(gz, 2), lax.rem(gy, 2)
    starts = (4, 8 - 8 * side, 8 * side)

    def place(frefs, row0):
        for k in range(3):
            fref, fbase = frefs[k]
            for i in range(4):
                for j in range(4):
                    c = i * 4 + j
                    row, col = row0 + i, starts[k] + j
                    f[row, col] = fref[fbase + c * R : fbase + (c + 1) * R, :]
                    s[row, col] = fref[fbase + 256 + c : fbase + 257 + c, :]

    place(((fown, 0), (feven, 0), (fodd, 0)), 4)
    for fref, row0 in ((fon, 8 - 8 * core), (foff, 8 * core)):
        place([(fref, 272 * k) for k in range(3)], row0)
    for i in range(4):
        for j in range(4):
            at = (i * 4 + j) * R
            for k, ref in enumerate((own, own_even, own_odd)):
                u[4 + i, starts[k] + j] = ref[at : at + R, :]
    for ref, left in ((on, core), (off, 1 - core)):
        for r in range(4):
            row = 8 + r - left * (5 + 2 * r)
            for j in range(4):
                at = (r * 4 + j) * R
                u[row, 4 + j] = ref[at : at + R, :]
        for m, (r, n) in enumerate(SIDE4):
            row = 8 + r - left * (5 + 2 * r)
            for k, across in enumerate((side, 1 - side)):
                at = (16 + k * len(SIDE4) + m) * R
                u[row, 8 + n - across * (5 + 2 * n)] = ref[at : at + R, :]

    def emit(i, j, value):
        lines[i - 3, j - 3] = value.astype(BF16)
        res[i, j] = value

    smooth(u, f, s, res, d0, d1, emit, 0, 6, 12, False)
    for i in range(4):
        for j in range(4):
            out[i, j] = res[4 + i, 4 + j]

    for copy in copies:
        copy.wait()

    def index(i, j, k):
        q = links[i, k, j]
        row = lax.rem(q // 16 - 4 * gz + 1 + 4 * NZ, 4 * NZ)
        return row, lax.rem(lax.rem(q, 16) - 4 * gy + 1 + 4 * NY, 4 * NY)

    def row_of_cells(i, carry):
        for j in range(8):
            start[i, j] = prolong_cell(lines, index, blocks, guess, i, j)
        return carry

    lax.fori_loop(0, 8, row_of_cells, 0)
    for i in range(8):
        for j in range(3):
            at = (i * 3 + j) * R
            even[at : at + R, :] = start[i, 5 - 5 * side + j]
            odd[at : at + R, :] = start[i, 5 * side + j]


SIDE3 = ((0, 0), (0, 1), (1, 0))
ROWS = (24 + 2 * len(SIDE3)) * R


def rows_kernel(start, even, odd, on, off):
    core, side = lax.rem(lax.axis_index("gz"), 2), lax.rem(lax.axis_index("gy"), 2)
    for ref, right in ((on, 1 - core), (off, core)):
        for r in range(3):
            row = r + right * (7 - 2 * r)
            for j in range(8):
                at = (r * 8 + j) * R
                ref[at : at + R, :] = start[row, j]
        for m, (r, n) in enumerate(SIDE3):
            row = r + right * (7 - 2 * r)
            for k, (beside, left) in enumerate(((even, side), (odd, 1 - side))):
                at = (24 + k * len(SIDE3) + m) * R
                ref[at : at + R, :] = at_cell(beside, row * 3 + n + left * (2 - 2 * n))


def first_kernel(own, even, odd, on, off, fown, sown, feven, fodd, fon, foff, out, u, f, s, res, d0, d1, done, sems):
    gz, gy = lax.axis_index("gz"), lax.axis_index("gy")
    core, side = lax.rem(gz, 2), lax.rem(gy, 2)
    even_u, odd_u = 11 - 11 * side, 11 * side
    even_f, odd_f = 11 - 10 * side, 1 + 10 * side

    for i in range(8):
        for j in range(8):
            u[3 + i, 3 + j] = own[i, j]
            f[3 + i, 3 + j] = fown[i, j]
            s[3 + i, 3 + j] = sown[i, j : j + 1, :]
        for j in range(3):
            at = (i * 3 + j) * R
            u[3 + i, even_u + j] = even[at : at + R, :]
            u[3 + i, odd_u + j] = odd[at : at + R, :]
        for j in range(2):
            c = i * 2 + j
            at = 272 + c * R
            f[3 + i, even_f + j] = feven[at : at + R, :]
            f[3 + i, odd_f + j] = fodd[at : at + R, :]
            s[3 + i, even_f + j] = feven[528 + c : 529 + c, :]
            s[3 + i, odd_f + j] = fodd[528 + c : 529 + c, :]

    def place(ref, fref, left, row_f):
        for r in range(3):
            for j in range(8):
                at = (r * 8 + j) * R
                u[11 + r - left * (9 + 2 * r), 3 + j] = ref[at : at + R, :]
        for m, (r, n) in enumerate(SIDE3):
            for k, across in enumerate((side, 1 - side)):
                at = (24 + k * len(SIDE3) + m) * R
                u[11 + r - left * (9 + 2 * r), 11 + n - across * (9 + 2 * n)] = ref[at : at + R, :]
        for i in range(2):
            for j in range(12):
                col = 3 + j if j < 8 else even_f + j - 8 if j < 10 else odd_f + j - 10
                c = i * 12 + j
                at = 816 + c * R
                f[row_f + i, col] = fref[at : at + R, :]
                s[row_f + i, col] = fref[1200 + c : 1201 + c, :]

    place(on, fon, core, 11 - 10 * core)
    place(off, foff, 1 - core, 1 + 10 * core)

    def emit(i, j, value):
        done[i - 3, j - 3] = value

    def leave(i):
        return pltpu.make_async_copy(done.at[i], out.at[i], sems.at[i])

    smooth(u, f, s, res, d0, d1, emit, 0, 8, 14, False, lambda i: leave(i - 3).start())
    for i in range(8):
        leave(i).wait()


def onchip(*shape):
    return pltpu.VMEM(shape, F32)


def sds(*shape, dtype=F32):
    return jax.ShapeDtypeStruct(shape, dtype)


def flat(x):
    return x.reshape(-1, L)


def shards(
    source_first, source_second, source_third, source_fourth,
    guess_first, guess_second, guess_third, guess_fourth,
    shift_first, shift_second, shift_third, shift_fourth,
    blocks_first, blocks_second, blocks_third,
    links_first, links_second, links_third,
):
    links_first, links_second = links_first.transpose(0, 2, 1), links_second.transpose(0, 2, 1)

    (pack,) = call(
        pack_kernel,
        (source_fourth, guess_fourth, shift_fourth, shift_third, source_third),
        (sds(104, L),),
        [pltpu.VMEM((1, 1, L), F32), pltpu.VMEM((2, 2, L), F32), pltpu.SemaphoreType.DMA((8,))],
        1000, 2, range(5),
    )
    y1 = y_by(pack, 1)
    y2 = y_by(pack, 2)
    y3 = y_by(pack, 3)
    line = jnp.stack([pack, y1, y2, y3])
    line_on = z_on(line)
    pair, short = call(pair_kernel, (line, line_on), (sds(2, 4, 104, L), sds(2, 4, 40, L)), [], 1000, 2)
    near = z_off(pair)
    far = z_off3(short)
    (both,) = call(relay_kernel, (near, far), (sds(2, 4, 144, L),), [], 1000, 3)
    both = z_on(both)

    third, mine, ahead_even, ahead_odd, row_low, row_high = call(
        ahead_kernel,
        (source_first, shift_first, source_second, shift_second, blocks_third, guess_third, links_third),
        (sds(THIRD, L, dtype=BF16), sds(272, L), sds(ALONG_Y, L), sds(ALONG_Y, L), sds(272, L), sds(272, L)),
        [pltpu.VMEM(x.shape, x.dtype) for x in (source_first, shift_first, source_second, shift_second, guess_third)]
        + [pltpu.SMEM(links_third.shape, jnp.int32), pltpu.SemaphoreType.DMA((16,))],
        1000, 6, range(7),
    )
    row_on, row_off = call(pick_kernel, (row_low, row_high), (sds(272, L), sds(272, L)), [], 1000, 2)
    third1 = y_by(third, 1)
    third2 = y_by(third, 2)
    third3 = y_by(third, 3)
    ahead_even = y_even(ahead_even)
    ahead_odd = y_odd(ahead_odd)
    ahead_on, ahead_off = call(
        along_z_kernel,
        (mine, ahead_even, ahead_odd, row_on, row_off),
        (sds(ALONG_Z, L), sds(ALONG_Z, L)),
        [], 10000, 6,
    )
    ahead_on = z_on(ahead_on)
    ahead_off = z_off(ahead_off)

    def smoothing_scratch(rows, cols):
        return [cells(rows, cols), cells(rows, cols), shifts(rows, cols)] + [cells(rows, cols)] * 3

    out_fourth, start_third = call(
        fourth_kernel,
        (pair, near, far, both, third, third1, third2, third3),
        (onchip(1, 1, R, L), sds(256, L)),
        smoothing_scratch(10, 4) + [cells(3, 4)],
        4_000_000, 6,
    )

    start_on = z_on(start_third)
    pair3 = jnp.stack([start_third, start_on])
    near3 = z_off(pair3)
    near3_b = z_on(near3)
    out_third, start_second = call(
        third_kernel,
        (pair3, near3, near3_b, pair, near, both, links_second, blocks_second, guess_second),
        (onchip(2, 2, R, L), sds(4, 4, R, L)),
        smoothing_scratch(12, 8) + [cells(4, 8, BF16)] + smem_last(guess_second, links_second),
        8_000_000, 12, (6, 8),
    )

    own = flat(start_second)
    own_even, own_odd = y_even(own), y_odd(own)
    block_on, block_off = call(block_kernel, (own, own_even, own_odd), (sds(BLOCK, L), sds(BLOCK, L)), [], 10000, 4)
    out_second, start_first, strip_even, strip_odd = call(
        second_kernel,
        (own, own_even, own_odd, z_on(block_on), z_off(block_off), mine, ahead_even, ahead_odd, ahead_on, ahead_off, links_first, blocks_first, guess_first),
        (onchip(4, 4, R, L), sds(8, 8, R, L), sds(24 * R, L), sds(24 * R, L)),
        smoothing_scratch(12, 12) + [cells(6, 6, BF16)] + smem_last(links_first),
        16_000_000, 20, (10,),
    )

    u_even, u_odd = y_even(strip_even), y_odd(strip_odd)
    u_on, u_off = call(rows_kernel, (start_first, u_even, u_odd), (sds(ROWS, L), sds(ROWS, L)), [], 10000, 4)
    (out_first,) = call(
        first_kernel,
        (start_first, u_even, u_odd, z_on(u_on), z_off(u_off), source_first, shift_first, ahead_even, ahead_odd, ahead_on, ahead_off),
        (sds(8, 8, R, L),),
        smoothing_scratch(14, 14) + [cells(8, 8), pltpu.SemaphoreType.DMA((8,))],
        16_000_000, 20, (), HBM,
    )
    return out_first, out_second, out_third, out_fourth


def solution(mesh):
    field = P("gz", "gy", None, None)
    line = P("gz", "gy", None)
    block = P("gz", "gy", None, None, None)

    return jax.shard_map(
        shards,
        mesh=mesh,
        in_specs=(field,) * 8 + (line,) * 4 + (block,) * 3 + (line,) * 3,
        out_specs=(field,) * 4,
        check_vma=False,
    )
```
